64 devices in a mesh: dp: 4 (over x, y), tp: 16 (over z, core).
Axes of the slice: x: 2, y: 2, z: 8, core: 2. Of those that a mesh axis runs over, the one named last changes fastest.
The devices are a block of a 4x4x8 slice.
Arguments:
- x: bfloat16 [8192, 4096], P('dp'), parts along dimension 0
- pos: int32 [8192], P('dp'), parts along dimension 0
- g1: bfloat16 [4096], replicated
- g2: bfloat16 [4096], replicated
- wq: bfloat16 [4096, 4096], P(None, 'tp')
- wk: bfloat16 [4096, 1024], replicated
- wv: bfloat16 [4096, 1024], replicated
- wo: bfloat16 [4096, 4096], P('tp')
- wg: bfloat16 [4096, 14336], P(None, 'tp')
- wu: bfloat16 [4096, 14336], P(None, 'tp')
- wd: bfloat16 [14336, 4096], P('tp')
Outputs:
- output 1: bfloat16 [8192, 4096], P('dp'), parts along dimension 0
- output 2: bfloat16 [8192, 16, 128], P('dp', 'tp'), parts along dimension 0
- output 3: bfloat16 [8192, 16, 128], P('dp', 'tp'), parts along dimension 0
There are 4 independent parts. The reference program is written for one: setup_inputs(seed, part) draws one part's arguments, and reference() takes and returns one part's arrays. A program takes and returns all parts, laid end to end along the dimension named above; an argument that names none is the same for every part.
All inputs are finite; a program needn't handle non-finite values.
Results may differ from the reference program's by a relative error of at most 0.019963.
Values are sent between devices in bfloat16 or wider.
A program may use at most 768 MiB of HBM per device.

```python
import jax
import jax.numpy as jnp
from jax import lax
import numpy as np

D = 4096
HEADS = 32
KV_HEADS = 8
HEAD = 128
FF = 14336
T = 2048
SLOTS = 16

EPS = 1e-5
ROPE_BASE = 500000.0
R = HEADS // KV_HEADS
QB = min(T, 256)


def setup_inputs(seed: int = 0, part: int = 0) -> dict:
    base = jax.random.PRNGKey(seed)
    kw = jax.random.split(jax.random.fold_in(base, 0), 9)
    kx, kp = jax.random.split(jax.random.fold_in(jax.random.fold_in(base, 1), part))

    def w(k, shape, scale):
        return (jax.random.normal(k, shape, jnp.float32) * scale).astype(jnp.bfloat16)

    def gain(k):
        return (1.0 + 0.2 * jax.random.normal(k, (D,), jnp.float32)).astype(jnp.bfloat16)

    x = jax.random.normal(kx, (T, D), jnp.float32).astype(jnp.bfloat16)
    pos = jax.random.randint(kp, (), 0, 4096, dtype=jnp.int32) + jnp.arange(T, dtype=jnp.int32)
    return {
        "x": x,
        "pos": pos,
        "g1": gain(kw[0]),
        "g2": gain(kw[1]),
        "wq": w(kw[2], (D, HEADS * HEAD), 1.5 * D ** -0.5),
        "wk": w(kw[3], (D, KV_HEADS * HEAD), 1.5 * D ** -0.5),
        "wv": w(kw[4], (D, KV_HEADS * HEAD), D ** -0.5),
        "wo": w(kw[5], (HEADS * HEAD, D), 2.0 * (HEADS * HEAD) ** -0.5),
        "wg": w(kw[6], (D, FF), D ** -0.5),
        "wu": w(kw[7], (D, FF), D ** -0.5),
        "wd": w(kw[8], (FF, D), 2.0 * FF ** -0.5),
    }


def _rms(x, g):
    x32 = x.astype(jnp.float32)
    inv = lax.rsqrt(jnp.mean(x32 * x32, axis=-1, keepdims=True) + EPS)
    return (x32 * inv * g.astype(jnp.float32)).astype(jnp.bfloat16)


def _rope(t, pos):
    half = HEAD // 2
    inv = ROPE_BASE ** (-2.0 * jnp.arange(half, dtype=jnp.float32) / HEAD)
    ang = pos.astype(jnp.float32)[:, None] * inv[None, :]
    c = jnp.cos(ang)[:, None, :]
    s = jnp.sin(ang)[:, None, :]
    t1, t2 = t[..., :half], t[..., half:]
    return jnp.concatenate([t1 * c - t2 * s, t2 * c + t1 * s], axis=-1)


def reference(x, pos, g1, g2, wq, wk, wv, wo, wg, wu, wd):
    a = _rms(x, g1)
    q = _rope(jnp.dot(a, wq, preferred_element_type=jnp.float32).reshape(T, HEADS, HEAD), pos).astype(jnp.bfloat16)
    k = _rope(jnp.dot(a, wk, preferred_element_type=jnp.float32).reshape(T, KV_HEADS, HEAD), pos).astype(jnp.bfloat16)
    v = jnp.dot(a, wv, preferred_element_type=jnp.float32).astype(jnp.bfloat16).reshape(T, KV_HEADS, HEAD)
    qg = q.reshape(T // QB, QB, KV_HEADS, R, HEAD)
    pq = pos.reshape(T // QB, QB)
    scale = HEAD ** -0.5

    def one_head(g):
        kg = k[:, g].astype(jnp.float32)
        vg = v[:, g].astype(jnp.float32)

        def one_block(blk):
            qq, pb = blk
            sc = jnp.einsum("qrd,kd->rqk", qq.astype(jnp.float32), kg) * scale
            sc = jnp.where((pos[None, :] <= pb[:, None])[None], sc, -jnp.inf)
            e = jnp.exp(sc - jnp.max(sc, axis=-1, keepdims=True))
            pr = (e / jnp.sum(e, axis=-1, keepdims=True)).astype(jnp.bfloat16)
            return jnp.einsum("rqk,kd->qrd", pr.astype(jnp.float32), vg).astype(jnp.bfloat16)

        return lax.map(one_block, (qg[:, :, g], pq))

    o = lax.map(one_head, jnp.arange(KV_HEADS))
    o = o.transpose(1, 2, 0, 3, 4).reshape(T, HEADS * HEAD)
    h = (x.astype(jnp.float32) + jnp.dot(o, wo, preferred_element_type=jnp.float32)).astype(jnp.bfloat16)
    b = _rms(h, g2)
    gt = jnp.dot(b, wg, preferred_element_type=jnp.float32)
    up = jnp.dot(b, wu, preferred_element_type=jnp.float32)
    u = (jax.nn.silu(gt) * up).astype(jnp.bfloat16)
    y = (h.astype(jnp.float32) + jnp.dot(u, wd, preferred_element_type=jnp.float32)).astype(jnp.bfloat16)
    sl = np.arange(SLOTS) * KV_HEADS // SLOTS
    return (y, k[:, sl], v[:, sl])
```

```python
import functools

import jax
import jax.numpy as jnp
from jax import lax
from jax.experimental import pallas as pl
from jax.experimental.pallas import tpu as pltpu
from jax.sharding import PartitionSpec as P

HEAD = 128
EPS = 1e-5
ROPE_BASE = 500000.0
SLOTS = 6
SUBS = 2
MESH = pl.DeviceIdType.MESH
F32, BF16 = jnp.float32, jnp.bfloat16


def _head_kernel(hd_ref, x_ref, g1_ref, cos_ref, sin_ref, wq_ref, wk_ref, wv_ref,
                 o_ref, k_ref, v_ref, wkv, a, ks, vs, sc):
    i = pl.program_id(0)
    qb = x_ref.shape[0]
    hl = wq_ref.shape[1] // HEAD

    @pl.when(i == 0)
    def _():
        wkv[:, :HEAD] = wk_ref[...]
        wkv[:, HEAD:] = wv_ref[...]

    rows = 16

    @pl.loop(0, qb // rows)
    def _(t):
        r = pl.ds(pl.multiple_of(t * rows, rows), rows)
        x32 = x_ref[r, :].astype(F32)
        inv = lax.rsqrt(jnp.mean(x32 * x32, axis=-1, keepdims=True) + EPS)
        a[r, :] = (x32 * inv * g1_ref[...].astype(F32)).astype(BF16)

    c, s = cos_ref[...], sin_ref[...]

    def rope(t):
        return (t * c + pltpu.roll(t, HEAD // 2, 1) * s).astype(BF16)

    kv = jnp.dot(a[...], wkv[...], preferred_element_type=F32)
    k = rope(kv[:, :HEAD])
    v = kv[:, HEAD:].astype(BF16)
    k_ref[...] = k
    v_ref[...] = v
    here = pl.ds(pl.multiple_of(i * qb, qb), qb)
    ks[here, :] = k
    vs[here, :] = v
    q = jnp.dot(a[...], wq_ref[...], preferred_element_type=F32)
    scale = HEAD ** -0.5

    for h in range(hl):
        qh = rope(q[:, h * HEAD:(h + 1) * HEAD])

        def scores(kb):
            kk = ks[pl.ds(pl.multiple_of(kb * qb, qb), qb), :]
            return lax.dot_general(qh, kk, (((1,), (1,)), ((), ())), preferred_element_type=F32) * scale

        def first(kb, mx):
            t = scores(kb)
            sc[kb] = t
            return jnp.maximum(mx, jnp.max(t, axis=-1, keepdims=True))

        t = scores(i)
        row = lax.broadcasted_iota(jnp.int32, t.shape, 0)
        col = lax.broadcasted_iota(jnp.int32, t.shape, 1)
        t = jnp.where(col <= row, t, -jnp.inf)
        sc[i] = t
        mx = lax.fori_loop(0, i, first, jnp.max(t, axis=-1, keepdims=True))

        def second(kb, total):
            e = jnp.exp(sc[kb] - mx)
            sc[kb] = e
            return total + jnp.sum(e, axis=-1, keepdims=True)

        total = lax.fori_loop(0, i + 1, second, jnp.zeros((qb, 1), F32))

        def third(kb, acc):
            pr = (sc[kb] / total).astype(BF16)
            vv = vs[pl.ds(pl.multiple_of(kb * qb, qb), qb), :]
            return acc + jnp.dot(pr, vv, preferred_element_type=F32)

        acc = lax.fori_loop(0, i + 1, third, jnp.zeros((qb, HEAD), F32))
        o_ref[:, h * HEAD:(h + 1) * HEAD] = acc.astype(BF16)


def _attention(head, x, g1, cos, sin, wq, wk, wv):
    t, d = x.shape
    qb = min(t, 256)
    hw = wq.shape[1]
    spec = pltpu.PrefetchScalarGridSpec(
        num_scalar_prefetch=1,
        grid=(t // qb,),
        in_specs=[
            pl.BlockSpec((qb, d), lambda i, hd: (i, 0)),
            pl.BlockSpec((1, d), lambda i, hd: (0, 0)),
            pl.BlockSpec((qb, HEAD), lambda i, hd: (i, 0)),
            pl.BlockSpec((qb, HEAD), lambda i, hd: (i, 0)),
            pl.BlockSpec((d, hw), lambda i, hd: (0, 0)),
            pl.BlockSpec((d, HEAD), lambda i, hd: (0, hd[0])),
            pl.BlockSpec((d, HEAD), lambda i, hd: (0, hd[0])),
        ],
        out_specs=[
            pl.BlockSpec((qb, hw), lambda i, hd: (i, 0)),
            pl.BlockSpec((qb, HEAD), lambda i, hd: (i, 0)),
            pl.BlockSpec((qb, HEAD), lambda i, hd: (i, 0)),
        ],
        scratch_shapes=[
            pltpu.VMEM((d, 2 * HEAD), BF16),
            pltpu.VMEM((qb, d), BF16),
            pltpu.VMEM((t, HEAD), BF16),
            pltpu.VMEM((t, HEAD), BF16),
            pltpu.VMEM((t // qb, qb, qb), F32),
        ],
    )
    return pl.pallas_call(
        _head_kernel,
        out_shape=(jax.ShapeDtypeStruct((t, hw), BF16), jax.ShapeDtypeStruct((t, HEAD), BF16),
                   jax.ShapeDtypeStruct((t, HEAD), BF16)),
        grid_spec=spec,
        compiler_params=pltpu.CompilerParams(
            dimension_semantics=("arbitrary",), vmem_limit_bytes=48 << 20),
        name="qkv_attention",
    )(head, x, g1, cos, sin, wq, wk, wv)


def _ring_kernel(n, o_hbm, x_hbm, g2_ref, wo_hbm, wg_hbm, wu_hbm, wd_hbm, y_hbm,
                 slots, stage, part, hown, u, o, wo, wgu, wd,
                 send_sem, recv_sem, in_sem, out_sem, own_sem, free_sem):
    me = lax.axis_index("tp")
    right, left = lax.rem(me + 1, n), lax.rem(me + n - 1, n)
    peer = (right, left)
    d_model = wo.shape[1]
    ff = wd.shape[0]
    blk = stage.shape[0]
    half = blk // 2
    sub = half // SUBS
    last = n - 2
    total_msgs = 4 * (n - 1)

    loads = [pltpu.make_async_copy(o_hbm, o, in_sem.at[0]),
             pltpu.make_async_copy(wo_hbm, wo, in_sem.at[1]),
             pltpu.make_async_copy(x_hbm.at[pl.ds(pl.multiple_of(me * blk, blk), blk)], hown, in_sem.at[2]),
             pltpu.make_async_copy(wd_hbm, wd, in_sem.at[3])]
    for i in range(ff // 128):
        c = pl.ds(i * 128, 128)
        loads.append(pltpu.make_async_copy(wg_hbm.at[:, c], wgu.at[:, pl.ds(i * 256, 128)], in_sem.at[4 + 2 * i]))
        loads.append(pltpu.make_async_copy(wu_hbm.at[:, c], wgu.at[:, pl.ds(i * 256 + 128, 128)], in_sem.at[5 + 2 * i]))
    for cp in loads:
        cp.start()

    barrier = pltpu.get_barrier_semaphore()
    for p in peer:
        pl.semaphore_signal(barrier, inc=1, device_id={"tp": p}, device_id_type=MESH)
    pl.semaphore_wait(barrier, 2)

    def rows(d, j):
        return pl.ds(d * half + j * sub, sub)

    def message(d, j, m, src=None):
        slot = lax.rem(m, SLOTS)
        dst = slots.at[slot, rows(d, j)]
        return pltpu.make_async_remote_copy(
            src_ref=dst if src is None else src, dst_ref=dst,
            send_sem=send_sem.at[d, j, slot], recv_sem=recv_sem.at[d, j, slot],
            device_id={"tp": peer[d]}, device_id_type=MESH)

    def when(cond, fn):
        if isinstance(cond, bool):
            if cond:
                fn()
        else:
            pl.when(cond)(fn)

    def take_credit(d, m):
        when(m >= SLOTS, lambda: pl.semaphore_wait(free_sem.at[d], 1))

    def give_credit(d, m):
        when(m <= total_msgs - 1 - SLOTS,
             lambda: pl.semaphore_signal(free_sem.at[d], inc=1, device_id={"tp": peer[1 - d]}, device_id_type=MESH))

    def sent(m):
        for d in range(2):
            for j in range(SUBS):
                message(d, j, m).wait_send()

    def forward(d, j, m, src):
        if j == 0:
            take_credit(d, m)
        message(d, j, m, src).start()

    def send_stage(m):
        for j in range(SUBS):
            for d in range(2):
                forward(d, j, m, stage.at[rows(d, j)])

    tile = min(512, d_model)

    def partial(lhs, w, top, bottom):
        @pl.loop(0, d_model // tile)
        def _(i):
            c = pl.ds(pl.multiple_of(i * tile, tile), tile)
            l = jnp.concatenate([lhs[pl.ds(pl.multiple_of(top * blk, blk), half), :],
                                 lhs[pl.ds(pl.multiple_of(bottom * blk + half, half), half), :]], axis=0)
            part[:, c] = jnp.dot(l, w[:, c], preferred_element_type=F32)

    def reduce_scatter(phase, lhs, w, finish):
        base = phase * (n - 1)
        partial(lhs, w, left, right)
        stage[...] = part[...].astype(BF16)
        send_stage(base)

        @pl.loop(0, last)
        def _(s):
            m = base + s
            slot = lax.rem(m, SLOTS)
            partial(lhs, w, lax.rem(me + 2 * n - s - 2, n), lax.rem(me + s + 2, n))
            for j in range(SUBS):
                for d in range(2):
                    message(d, j, m).wait_recv()
                    ref = slots.at[slot, rows(d, j)]
                    ref[...] = (ref[...].astype(F32) + part[d * half + j * sub:d * half + (j + 1) * sub, :]).astype(BF16)
                    forward(d, j, m + 1, ref)
            sent(m)

            @pl.when(s >= 1)
            def _():
                for d in range(2):
                    give_credit(d, m - 1)

        m = base + last
        partial(lhs, w, me, me)
        sent(m)
        for d in range(2):
            give_credit(d, m - 1)
        for j in range(SUBS):
            for d in range(2):
                message(d, j, m).wait_recv()
                r = slice(d * half + j * sub, d * half + (j + 1) * sub)
                finish(r, slots[m % SLOTS, r, :].astype(F32) + part[r, :])
        for d in range(2):
            give_credit(d, m)

    def all_gather(phase, own, arrived, settle):
        base = phase * (n - 1)
        send_stage(base)
        own()

        @pl.loop(0, last)
        def _(s):
            m = base + s
            slot = lax.rem(m, SLOTS)
            for j in range(SUBS):
                for d in range(2):
                    message(d, j, m).wait_recv()
                    forward(d, j, m + 1, slots.at[slot, rows(d, j)])
            arrived(m, slot, lax.rem(me + n - s - 1, n), lax.rem(me + s + 1, n))
            sent(m)

            @pl.when(s >= 1)
            def _():
                settle(m - 1)
                for d in range(2):
                    give_credit(d, m - 1)

        m = base + last
        for j in range(SUBS):
            for d in range(2):
                message(d, j, m).wait_recv()
        arrived(m, m % SLOTS, right, left)
        sent(m)
        for q in (m - 1, m):
            settle(q)
            for d in range(2):
                give_credit(d, q)

    for cp in loads[:3]:
        cp.wait()

    def finish_h(r, total):
        h = (hown[r, :].astype(F32) + total).astype(BF16)
        hown[r, :] = h
        h32 = h.astype(F32)
        inv = lax.rsqrt(jnp.mean(h32 * h32, axis=-1, keepdims=True) + EPS)
        stage[r, :] = (h32 * inv * g2_ref[...].astype(F32)).astype(BF16)

    reduce_scatter(0, o, wo, finish_h)

    for cp in loads[3:]:
        cp.wait()

    def gate_up(b_ref, top, bottom):
        @pl.loop(0, ff // 128)
        def _(i):
            gu = jnp.dot(b_ref[...], wgu[:, pl.ds(pl.multiple_of(i * 256, 256), 256)], preferred_element_type=F32)
            g, up = gu[:, :128], gu[:, 128:]
            val = (jax.nn.silu(g) * up).astype(BF16)
            c = pl.ds(pl.multiple_of(i * 128, 128), 128)
            u[pl.ds(pl.multiple_of(top * blk, blk), half), c] = val[:half]
            u[pl.ds(pl.multiple_of(bottom * blk + half, half), half), c] = val[half:]

    all_gather(1, lambda: gate_up(stage, me, me),
               lambda m, slot, top, bottom: gate_up(slots.at[slot], top, bottom), lambda m: None)

    def finish_y(r, total):
        stage[r, :] = (hown[r, :].astype(F32) + total).astype(BF16)

    reduce_scatter(2, u, wd, finish_y)

    own = pltpu.make_async_copy(stage, y_hbm.at[pl.ds(pl.multiple_of(me * blk, blk), blk)], own_sem)

    def out(m, d, block):
        slot = lax.rem(m, SLOTS)
        return pltpu.make_async_copy(
            slots.at[slot, pl.ds(d * half, half)],
            y_hbm.at[pl.ds(pl.multiple_of(block * blk + d * half, half), half)], out_sem.at[d, slot])

    def arrived_y(m, slot, top, bottom):
        out(m, 0, top).start()
        out(m, 1, bottom).start()

    def settle_y(m):
        for d in range(2):
            out(m, d, me).wait()

    all_gather(3, own.start, arrived_y, settle_y)
    own.wait()


def _ring(n, o, x, g2, wo, wg, wu, wd):
    t, d = x.shape
    ff = wd.shape[0]
    blk = t // n
    hbm = pl.BlockSpec(memory_space=pl.ANY)
    dma = pltpu.SemaphoreType.DMA
    return pl.pallas_call(
        functools.partial(_ring_kernel, n),
        out_shape=jax.ShapeDtypeStruct((t, d), BF16),
        in_specs=[hbm, hbm, pl.BlockSpec(memory_space=pltpu.VMEM), hbm, hbm, hbm, hbm],
        out_specs=hbm,
        scratch_shapes=[
            pltpu.VMEM((SLOTS, blk, d), BF16),
            pltpu.VMEM((blk, d), BF16),
            pltpu.VMEM((blk, d), F32),
            pltpu.VMEM((blk, d), BF16),
            pltpu.VMEM((t, ff), BF16),
            pltpu.VMEM(o.shape, BF16),
            pltpu.VMEM(wo.shape, BF16),
            pltpu.VMEM((d, 2 * ff), BF16),
            pltpu.VMEM(wd.shape, BF16),
            dma((2, SUBS, SLOTS)),
            dma((2, SUBS, SLOTS)),
            dma((4 + 2 * (ff // 128),)),
            dma((2, SLOTS)),
            dma,
            pltpu.SemaphoreType.REGULAR((2,)),
        ],
        compiler_params=pltpu.CompilerParams(
            collective_id=0, has_side_effects=True, vmem_limit_bytes=60 << 20),
        name="ring_layer",
    )(o, x, g2, wo, wg, wu, wd)


def solution(mesh):
    tp = mesh.shape["tp"]

    def local(x, pos, g1, g2, wq, wk, wv, wo, wg, wu, wd):
        t, d = x.shape
        g = wk.shape[1] // HEAD
        r = lax.axis_index("tp")
        head = (r * g // tp).astype(jnp.int32).reshape(1)
        half = HEAD // 2
        inv = ROPE_BASE ** (-2.0 * jnp.arange(half, dtype=F32) / HEAD)
        ang = pos.astype(F32)[:, None] * inv
        c, s = jnp.cos(ang), jnp.sin(ang)
        cos = jnp.concatenate([c, c], axis=-1)
        sin = jnp.concatenate([-s, s], axis=-1)
        o, k, v = _attention(head, x, g1.reshape(1, d), cos, sin, wq, wk, wv)
        y = _ring(tp, o, x, g2.reshape(1, d), wo, wg, wu, wd)
        return y, k.reshape(t, 1, HEAD), v.reshape(t, 1, HEAD)

    return jax.shard_map(
        local,
        mesh=mesh,
        in_specs=(P("dp", None), P("dp"), P(), P(), P(None, "tp"), P(), P(), P("tp", None),
                  P(None, "tp"), P(None, "tp"), P("tp", None)),
        out_specs=(P("dp", None), P("dp", "tp", None), P("dp", "tp", None)),
        check_vma=False,
    )
```

```python
import functools

import jax
import jax.numpy as jnp
from jax import lax
from jax.experimental import pallas as pl
from jax.experimental.pallas import tpu as pltpu
from jax.sharding import PartitionSpec as P

HEAD = 128
EPS = 1e-5
ROPE_BASE = 500000.0
SLOTS = 6
SUBS = 2
MESH = pl.DeviceIdType.MESH
F32, BF16 = jnp.float32, jnp.bfloat16


def _qkv_kernel(hd_ref, x_ref, g1_ref, cos_ref, sin_ref, wq_ref, wk_ref, wv_ref,
                q_ref, k_ref, v_ref, wkv, a):
    qb = x_ref.shape[0]
    hl = wq_ref.shape[1] // HEAD

    @pl.when(pl.program_id(0) == 0)
    def _():
        wkv[:, :HEAD] = wk_ref[...]
        wkv[:, HEAD:] = wv_ref[...]

    rows = 16

    @pl.loop(0, qb // rows)
    def _(t):
        r = pl.ds(pl.multiple_of(t * rows, rows), rows)
        x32 = x_ref[r, :].astype(F32)
        inv = lax.rsqrt(jnp.mean(x32 * x32, axis=-1, keepdims=True) + EPS)
        a[r, :] = (x32 * inv * g1_ref[...].astype(F32)).astype(BF16)

    c, s = cos_ref[...], sin_ref[...]

    def rope(t):
        return (t * c + pltpu.roll(t, HEAD // 2, 1) * s).astype(BF16)

    kv = jnp.dot(a[...], wkv[...], preferred_element_type=F32)
    k_ref[...] = rope(kv[:, :HEAD])
    v_ref[...] = kv[:, HEAD:].astype(BF16)
    q = jnp.dot(a[...], wq_ref[...], preferred_element_type=F32)
    for h in range(hl):
        q_ref[:, h * HEAD:(h + 1) * HEAD] = rope(q[:, h * HEAD:(h + 1) * HEAD])


def _qkv(head, x, g1, cos, sin, wq, wk, wv):
    t, d = x.shape
    qb = min(t, 256)
    hw = wq.shape[1]
    spec = pltpu.PrefetchScalarGridSpec(
        num_scalar_prefetch=1,
        grid=(t // qb,),
        in_specs=[
            pl.BlockSpec((qb, d), lambda i, hd: (i, 0)),
            pl.BlockSpec((1, d), lambda i, hd: (0, 0)),
            pl.BlockSpec((qb, HEAD), lambda i, hd: (i, 0)),
            pl.BlockSpec((qb, HEAD), lambda i, hd: (i, 0)),
            pl.BlockSpec((d, hw), lambda i, hd: (0, 0)),
            pl.BlockSpec((d, HEAD), lambda i, hd: (0, hd[0])),
            pl.BlockSpec((d, HEAD), lambda i, hd: (0, hd[0])),
        ],
        out_specs=[
            pl.BlockSpec((qb, hw), lambda i, hd: (i, 0)),
            pl.BlockSpec((qb, HEAD), lambda i, hd: (i, 0)),
            pl.BlockSpec((qb, HEAD), lambda i, hd: (i, 0)),
        ],
        scratch_shapes=[
            pltpu.VMEM((d, 2 * HEAD), BF16),
            pltpu.VMEM((qb, d), BF16),
        ],
    )
    return pl.pallas_call(
        _qkv_kernel,
        out_shape=(jax.ShapeDtypeStruct((t, hw), BF16), jax.ShapeDtypeStruct((t, HEAD), BF16),
                   jax.ShapeDtypeStruct((t, HEAD), BF16)),
        grid_spec=spec,
        compiler_params=pltpu.CompilerParams(
            dimension_semantics=("arbitrary",), vmem_limit_bytes=48 << 20),
        name="qkv",
    )(head, x, g1, cos, sin, wq, wk, wv)


def _ring_kernel(n, q_hbm, k_hbm, v_hbm, x_hbm, g2_ref, wo_hbm, wg_hbm, wu_hbm, wd_hbm, y_hbm,
                 slots, early, stage, part, hown, u, q, k, v, sc, orow, wo, wgu, wd,
                 send_sem, recv_sem, early_send, early_recv, in_sem, out_sem, own_sem, free_sem):
    me = lax.axis_index("tp")
    right, left = lax.rem(me + 1, n), lax.rem(me + n - 1, n)
    peer = (right, left)
    odd = lax.rem(me, 2)
    leaves = (odd == 1, odd == 0)
    stays = (odd == 0, odd == 1)
    d_model = wo.shape[1]
    ff = wd.shape[0]
    t_all = q.shape[0]
    heads = q.shape[1] // HEAD
    blk = stage.shape[0]
    half = blk // 2
    sub = half // SUBS
    last = n - 2
    total_msgs = 4 * (n - 1)
    pairs = [(j, d) for j in range(SUBS) for d in range(2)]

    loads = [pltpu.make_async_copy(src, dst, in_sem.at[i]) for i, (src, dst) in enumerate([
        (q_hbm, q), (k_hbm, k), (v_hbm, v), (wo_hbm, wo),
        (x_hbm.at[pl.ds(pl.multiple_of(me * blk, blk), blk)], hown), (wd_hbm, wd)])]
    for i in range(ff // 128):
        c = pl.ds(i * 128, 128)
        loads.append(pltpu.make_async_copy(wg_hbm.at[:, c], wgu.at[:, pl.ds(i * 256, 128)], in_sem.at[6 + 2 * i]))
        loads.append(pltpu.make_async_copy(wu_hbm.at[:, c], wgu.at[:, pl.ds(i * 256 + 128, 128)], in_sem.at[7 + 2 * i]))
    for cp in loads:
        cp.start()

    barrier = pltpu.get_barrier_semaphore()
    for p in peer:
        pl.semaphore_signal(barrier, inc=1, device_id={"tp": p}, device_id_type=MESH)
    pl.semaphore_wait(barrier, 2)

    def rows(d, j):
        return pl.ds(d * half + j * sub, sub)

    def span(d, j):
        return slice(d * half + j * sub, d * half + (j + 1) * sub)

    def message(d, j, m, src=None):
        slot = lax.rem(m, SLOTS)
        dst = slots.at[slot, rows(d, j)]
        return pltpu.make_async_remote_copy(
            src_ref=dst if src is None else src, dst_ref=dst,
            send_sem=send_sem.at[d, j, slot], recv_sem=recv_sem.at[d, j, slot],
            device_id={"tp": peer[d]}, device_id_type=MESH)

    def direct(d, j, phase):
        return pltpu.make_async_remote_copy(
            src_ref=stage.at[rows(d, j)], dst_ref=early.at[phase, pl.ds(j * sub, sub)],
            send_sem=early_send.at[phase, j], recv_sem=early_recv.at[phase, j],
            device_id={"tp": peer[1 - d]}, device_id_type=MESH)

    def when(cond, fn):
        if isinstance(cond, bool):
            if cond:
                fn()
        else:
            pl.when(cond)(fn)

    def take_credit(d, m):
        when(m >= SLOTS, lambda: pl.semaphore_wait(free_sem.at[d], 1))

    def give_credit(m):
        for d in range(2):
            when(m <= total_msgs - 1 - SLOTS, functools.partial(
                pl.semaphore_signal, free_sem.at[d], inc=1, device_id={"tp": peer[1 - d]}, device_id_type=MESH))

    tile = min(512, d_model)

    def project(lhs, w):
        @pl.loop(0, d_model // tile)
        def _(i):
            c = pl.ds(pl.multiple_of(i * tile, tile), tile)
            part[:, c] = jnp.dot(lhs(), w[:, c], preferred_element_type=F32)

    def reduce_start(phase, partial):
        base = phase * (n - 1)
        partial(left, right)
        stage[...] = part[...].astype(BF16)
        for j, d in pairs:
            if j == 0:
                take_credit(d, base)
            pl.when(leaves[d])(lambda d=d, j=j: direct(d, j, phase).start())
            pl.when(stays[d])(lambda d=d, j=j: message(d, j, base, stage.at[rows(d, j)]).start())

    def reduce_scatter(phase, partial, finish):
        base = phase * (n - 1)

        @pl.loop(0, last)
        def _(s):
            m = base + s
            slot = lax.rem(m, SLOTS)
            partial(lax.rem(me + 2 * n - s - 2, n), lax.rem(me + s + 2, n))
            for j, d in pairs:
                ref = slots.at[slot, rows(d, j)]
                opens = jnp.logical_and(s == 0, stays[d])

                @pl.when(opens)
                def _():
                    ref[...] = part[span(d, j), :].astype(BF16)

                @pl.when(jnp.logical_not(opens))
                def _():
                    message(d, j, m).wait_recv()
                    ref[...] = (ref[...].astype(F32) + part[span(d, j), :]).astype(BF16)

                if j == 0:
                    take_credit(d, m + 1)
                message(d, j, m + 1, ref).start()
            for j, d in pairs:
                handed = jnp.logical_and(s == 0, leaves[d])
                pl.when(handed)(lambda d=d, j=j: direct(d, j, phase).wait_send())
                pl.when(jnp.logical_not(handed))(lambda d=d, j=j: message(d, j, m).wait_send())
            pl.when(s >= 1)(lambda: give_credit(m - 1))

        m = base + last
        partial(me, me)
        for j, d in pairs:
            message(d, j, m).wait_send()
        give_credit(m - 1)
        for j, d in pairs:
            @pl.when(stays[d])
            def _():
                direct(d, j, phase).wait_recv()
                part[span(d, j), :] = part[span(d, j), :] + early[phase, j * sub:(j + 1) * sub, :].astype(F32)
        for j, d in pairs:
            message(d, j, m).wait_recv()
            r = span(d, j)
            finish(r, slots[m % SLOTS, r, :].astype(F32) + part[r, :])
            if j == 0:
                take_credit(d, m + 1)
            message(d, j, m + 1, stage.at[rows(d, j)]).start()
            pl.when(leaves[d])(lambda d=d, j=j: direct(d, j, phase + 1).start())
        give_credit(m)

    def all_gather(phase, own, arrived, settle, then):
        base = phase * (n - 1)
        own()

        @pl.loop(0, last)
        def _(s):
            m = base + s
            slot = lax.rem(m, SLOTS)
            for j, d in pairs:
                message(d, j, m).wait_recv()
                if j == 0:
                    take_credit(d, m + 1)
                pl.when(jnp.logical_or(s < last - 1, stays[d]))(
                    lambda d=d, j=j: message(d, j, m + 1, slots.at[slot, rows(d, j)]).start())
            arrived(m, slot, lax.rem(me + n - s - 1, n), lax.rem(me + s + 1, n))
            for j, d in pairs:
                message(d, j, m).wait_send()
                pl.when(jnp.logical_and(s == 0, leaves[d]))(lambda d=d, j=j: direct(d, j, phase).wait_send())

            @pl.when(s >= 1)
            def _():
                settle(m - 1)
                give_credit(m - 1)

        then()
        m = base + last
        for j, d in pairs:
            pl.when(stays[d])(lambda d=d, j=j: message(d, j, m).wait_send())
        settle(m - 1)
        give_credit(m - 1)
        for j, d in pairs:
            @pl.when(leaves[d])
            def _():
                message(d, j, m).wait_recv()

            @pl.when(stays[d])
            def _():
                direct(d, j, phase).wait_recv()
                slots[m % SLOTS, span(d, j), :] = early[phase, j * sub:(j + 1) * sub, :]
        arrived(m, m % SLOTS, right, left)
        settle(m)
        give_credit(m)

    kt = min(256, t_all)
    scale = HEAD ** -0.5
    lanes = kt // 128

    def attend(top, bottom):
        r0 = pl.multiple_of(top * blk, half)
        r1 = pl.multiple_of(bottom * blk + half, half)
        qa, qb = q[pl.ds(r0, half), :], q[pl.ds(r1, half), :]
        qq = jnp.concatenate([t[:, h * HEAD:(h + 1) * HEAD] for t in (qa, qb) for h in range(heads)], axis=0)
        i = lax.broadcasted_iota(jnp.int32, (2 * heads * half, kt), 0)
        row = jnp.where(i < heads * half, r0, r1) + (i & (half - 1))
        ahead = row - lax.broadcasted_iota(jnp.int32, row.shape, 1)
        mx = None
        for b in range(t_all // kt):
            c = slice(b * kt, (b + 1) * kt)
            t = lax.dot_general(qq, k[c, :], (((1,), (1,)), ((), ())), preferred_element_type=F32) * scale
            t = jnp.where(ahead >= b * kt, t, -jnp.inf)
            sc[:, c] = t
            for z in range(lanes):
                g = t[:, z * 128:(z + 1) * 128]
                mx = g if mx is None else jnp.maximum(mx, g)
        mx = jnp.max(mx, axis=-1, keepdims=True)
        tot = None
        for b in range(t_all // kt):
            c = slice(b * kt, (b + 1) * kt)
            e = jnp.exp(sc[:, c] - mx)
            sc[:, c] = e
            for z in range(lanes):
                g = e[:, z * 128:(z + 1) * 128]
                tot = g if tot is None else tot + g
        rinv = 1.0 / jnp.sum(tot, axis=-1, keepdims=True)
        acc = None
        for b in range(t_all // kt):
            c = slice(b * kt, (b + 1) * kt)
            pr = (sc[:, c] * rinv).astype(BF16)
            g = jnp.dot(pr, v[c, :], preferred_element_type=F32)
            acc = g if acc is None else acc + g
        for z in range(2):
            for h in range(heads):
                w = z * heads + h
                orow[z * half:(z + 1) * half, h * HEAD:(h + 1) * HEAD] = acc[w * half:(w + 1) * half].astype(BF16)

    def partial_o(top, bottom):
        attend(top, bottom)
        project(lambda: orow[...], wo)

    for cp in loads[:5]:
        cp.wait()

    def finish_h(r, total):
        h = (hown[r, :].astype(F32) + total).astype(BF16)
        hown[r, :] = h
        h32 = h.astype(F32)
        inv = lax.rsqrt(jnp.mean(h32 * h32, axis=-1, keepdims=True) + EPS)
        stage[r, :] = (h32 * inv * g2_ref[...].astype(F32)).astype(BF16)

    reduce_start(0, partial_o)
    reduce_scatter(0, partial_o, finish_h)

    for cp in loads[5:]:
        cp.wait()

    def gate_up(b_ref, top, bottom):
        @pl.loop(0, ff // 128)
        def _(i):
            gu = jnp.dot(b_ref[...], wgu[:, pl.ds(pl.multiple_of(i * 256, 256), 256)], preferred_element_type=F32)
            g, up = gu[:, :128], gu[:, 128:]
            val = (jax.nn.silu(g) * up).astype(BF16)
            c = pl.ds(pl.multiple_of(i * 128, 128), 128)
            u[pl.ds(pl.multiple_of(top * blk, blk), half), c] = val[:half]
            u[pl.ds(pl.multiple_of(bottom * blk + half, half), half), c] = val[half:]

    def partial_d(top, bottom):
        project(lambda: jnp.concatenate([u[pl.ds(pl.multiple_of(top * blk, blk), half), :],
                                         u[pl.ds(pl.multiple_of(bottom * blk + half, half), half), :]], axis=0), wd)

    all_gather(1, lambda: gate_up(stage, me, me),
               lambda m, slot, top, bottom: gate_up(slots.at[slot], top, bottom), lambda m: None,
               lambda: reduce_start(2, partial_d))

    def finish_y(r, total):
        stage[r, :] = (hown[r, :].astype(F32) + total).astype(BF16)

    reduce_scatter(2, partial_d, finish_y)

    own = pltpu.make_async_copy(stage, y_hbm.at[pl.ds(pl.multiple_of(me * blk, blk), blk)], own_sem)

    def out(m, d, block):
        slot = lax.rem(m, SLOTS)
        return pltpu.make_async_copy(
            slots.at[slot, pl.ds(d * half, half)],
            y_hbm.at[pl.ds(pl.multiple_of(block * blk + d * half, half), half)], out_sem.at[d, slot])

    def arrived_y(m, slot, top, bottom):
        out(m, 0, top).start()
        out(m, 1, bottom).start()

    def settle_y(m):
        for d in range(2):
            out(m, d, me).wait()

    all_gather(3, own.start, arrived_y, settle_y, lambda: None)
    own.wait()


def _ring(n, q, k, v, x, g2, wo, wg, wu, wd):
    t, d = x.shape
    ff = wd.shape[0]
    blk = t // n
    hbm = pl.BlockSpec(memory_space=pl.ANY)
    dma = pltpu.SemaphoreType.DMA
    return pl.pallas_call(
        functools.partial(_ring_kernel, n),
        out_shape=jax.ShapeDtypeStruct((t, d), BF16),
        in_specs=[hbm] * 4 + [pl.BlockSpec(memory_space=pltpu.VMEM)] + [hbm] * 4,
        out_specs=hbm,
        scratch_shapes=[
            pltpu.VMEM((SLOTS, blk, d), BF16),
            pltpu.VMEM((4, blk // 2, d), BF16),
            pltpu.VMEM((blk, d), BF16),
            pltpu.VMEM((blk, d), F32),
            pltpu.VMEM((blk, d), BF16),
            pltpu.VMEM((t, ff), BF16),
            pltpu.VMEM(q.shape, BF16),
            pltpu.VMEM(k.shape, BF16),
            pltpu.VMEM(v.shape, BF16),
            pltpu.VMEM((blk * (q.shape[1] // HEAD), t), F32),
            pltpu.VMEM((blk, q.shape[1]), BF16),
            pltpu.VMEM(wo.shape, BF16),
            pltpu.VMEM((d, 2 * ff), BF16),
            pltpu.VMEM(wd.shape, BF16),
            dma((2, SUBS, SLOTS)),
            dma((2, SUBS, SLOTS)),
            dma((4, SUBS)),
            dma((4, SUBS)),
            dma((6 + 2 * (ff // 128),)),
            dma((2, SLOTS)),
            dma,
            pltpu.SemaphoreType.REGULAR((2,)),
        ],
        compiler_params=pltpu.CompilerParams(
            collective_id=0, has_side_effects=True, vmem_limit_bytes=60 << 20),
        name="ring_layer",
    )(q, k, v, x, g2, wo, wg, wu, wd)


def solution(mesh):
    tp = mesh.shape["tp"]

    def local(x, pos, g1, g2, wq, wk, wv, wo, wg, wu, wd):
        t, d = x.shape
        g = wk.shape[1] // HEAD
        r = lax.axis_index("tp")
        head = (r * g // tp).astype(jnp.int32).reshape(1)
        half = HEAD // 2
        inv = ROPE_BASE ** (-2.0 * jnp.arange(half, dtype=F32) / HEAD)
        ang = pos.astype(F32)[:, None] * inv
        c, s = jnp.cos(ang), jnp.sin(ang)
        cos = jnp.concatenate([c, c], axis=-1)
        sin = jnp.concatenate([-s, s], axis=-1)
        q, k, v = _qkv(head, x, g1.reshape(1, d), cos, sin, wq, wk, wv)
        y = _ring(tp, q, k, v, x, g2.reshape(1, d), wo, wg, wu, wd)
        return y, k.reshape(t, 1, HEAD), v.reshape(t, 1, HEAD)

    return jax.shard_map(
        local,
        mesh=mesh,
        in_specs=(P("dp", None), P("dp"), P(), P(), P(None, "tp"), P(), P(), P("tp", None),
                  P(None, "tp"), P(None, "tp"), P("tp", None)),
        out_specs=(P("dp", None), P("dp", "tp", None), P("dp", "tp", None)),
        check_vma=False,
    )
```

```python
import functools

import jax
import jax.numpy as jnp
from jax import lax
from jax.experimental import pallas as pl
from jax.experimental.pallas import tpu as pltpu
from jax.sharding import PartitionSpec as P

HEAD = 128
EPS = 1e-5
ROPE_BASE = 500000.0
SLOTS = 6
SUBS = 2
MESH = pl.DeviceIdType.MESH
F32, BF16 = jnp.float32, jnp.bfloat16


def _qkv_kernel(hd_ref, x_ref, g1_ref, cos_ref, sin_ref, wq_ref, wk_ref, wv_ref,
                q_ref, k_ref, v_ref, wkv, a0, a1):
    i = pl.program_id(0)
    steps = pl.num_programs(0)
    hb, d = a0.shape
    hl = wq_ref.shape[1] // HEAD
    chunks = 4
    rows = hb // chunks
    kd = d // chunks

    def norm(x0, a, z):
        r = slice(x0 + z * rows, x0 + (z + 1) * rows)
        o = slice(z * rows, (z + 1) * rows)
        ss = None
        for t in range(d // 128):
            x32 = x_ref[r, t * 128:(t + 1) * 128].astype(F32)
            ss = x32 * x32 if ss is None else ss + x32 * x32
        inv = lax.rsqrt(jnp.sum(ss, axis=-1, keepdims=True) * (1.0 / d) + EPS)
        for t in range(d // 128):
            c = slice(t * 128, (t + 1) * 128)
            a[o, c] = (x_ref[r, c].astype(F32) * inv * g1_ref[:, c].astype(F32)).astype(BF16)

    def work(a, at, x0=None, into=None):
        kv = q = None
        for z in range(chunks):
            kk = slice(z * kd, (z + 1) * kd)
            t = jnp.dot(a[:, kk], wkv[kk, :], preferred_element_type=F32)
            kv = t if kv is None else kv + t
            t = jnp.dot(a[:, kk], wq_ref[kk, :], preferred_element_type=F32)
            q = t if q is None else q + t
            if into is not None:
                norm(x0, into, z)
        here = pl.ds(pl.multiple_of(at, hb), hb)
        c, s = cos_ref[here, :], sin_ref[here, :]

        def rope(t):
            return (t * c + pltpu.roll(t, HEAD // 2, 1) * s).astype(BF16)

        k_ref[here, :] = rope(kv[:, :HEAD])
        v_ref[here, :] = kv[:, HEAD:].astype(BF16)
        for h in range(hl):
            q_ref[here, h * HEAD:(h + 1) * HEAD] = rope(q[:, h * HEAD:(h + 1) * HEAD])

    @pl.when(i == 0)
    def _():
        wkv[:, :HEAD] = wk_ref[...]
        wkv[:, HEAD:] = wv_ref[...]
        for z in range(chunks):
            norm(0, a0, z)

    @pl.when(jnp.logical_and(i > 0, i < steps - 1))
    def _():
        work(a1, (2 * i - 1) * hb, 0, a0)

    @pl.when(i < steps - 1)
    def _():
        work(a0, 2 * i * hb, hb, a1)

    @pl.when(i == steps - 1)
    def _():
        work(a1, (2 * i - 1) * hb)


def _qkv(head, x, g1, cos, sin, wq, wk, wv):
    t, d = x.shape
    hb = min(t // 4, 256)
    nb = t // (2 * hb)
    hw = wq.shape[1]
    spec = pltpu.PrefetchScalarGridSpec(
        num_scalar_prefetch=1,
        grid=(nb + 1,),
        in_specs=[
            pl.BlockSpec((2 * hb, d), lambda i, hd: (jnp.minimum(i, nb - 1), 0)),
            pl.BlockSpec((1, d), lambda i, hd: (0, 0)),
            pl.BlockSpec((t, HEAD), lambda i, hd: (0, 0)),
            pl.BlockSpec((t, HEAD), lambda i, hd: (0, 0)),
            pl.BlockSpec((d, hw), lambda i, hd: (0, 0)),
            pl.BlockSpec((d, HEAD), lambda i, hd: (0, hd[0])),
            pl.BlockSpec((d, HEAD), lambda i, hd: (0, hd[0])),
        ],
        out_specs=[
            pl.BlockSpec((t, hw), lambda i, hd: (0, 0)),
            pl.BlockSpec((t, HEAD), lambda i, hd: (0, 0)),
            pl.BlockSpec((t, HEAD), lambda i, hd: (0, 0)),
        ],
        scratch_shapes=[
            pltpu.VMEM((d, 2 * HEAD), BF16),
            pltpu.VMEM((hb, d), BF16),
            pltpu.VMEM((hb, d), BF16),
        ],
    )
    return pl.pallas_call(
        _qkv_kernel,
        out_shape=(jax.ShapeDtypeStruct((t, hw), BF16), jax.ShapeDtypeStruct((t, HEAD), BF16),
                   jax.ShapeDtypeStruct((t, HEAD), BF16)),
        grid_spec=spec,
        compiler_params=pltpu.CompilerParams(
            dimension_semantics=("arbitrary",), vmem_limit_bytes=48 << 20),
        name="qkv",
    )(head, x, g1, cos, sin, wq, wk, wv)


def _ring_kernel(n, q_hbm, k_hbm, v_hbm, x_hbm, g2_ref, wo_hbm, wg_hbm, wu_hbm, wd_hbm, y_hbm,
                 slots, early, stage, part, hown, u, q, k, v, sc, top_score, orow, wo, wgu, wd,
                 send_sem, recv_sem, early_send, early_recv, in_sem, out_sem, own_sem, free_sem):
    me = lax.axis_index("tp")
    right, left = lax.rem(me + 1, n), lax.rem(me + n - 1, n)
    peer = (right, left)
    odd = lax.rem(me, 2)
    leaves = (odd == 1, odd == 0)
    stays = (odd == 0, odd == 1)
    d_model = wo.shape[1]
    ff = wd.shape[0]
    t_all = q.shape[0]
    heads = q.shape[1] // HEAD
    blk = stage.shape[0]
    half = blk // 2
    sub = half // SUBS
    last = n - 2
    total_msgs = 4 * (n - 1)
    pairs = [(j, d) for j in range(SUBS) for d in range(2)]

    loads = [pltpu.make_async_copy(src, dst, in_sem.at[i]) for i, (src, dst) in enumerate([
        (q_hbm, q), (k_hbm, k), (v_hbm, v), (wo_hbm, wo),
        (x_hbm.at[pl.ds(pl.multiple_of(me * blk, blk), blk)], hown), (wd_hbm, wd)])]
    for i in range(ff // 128):
        c = pl.ds(i * 128, 128)
        loads.append(pltpu.make_async_copy(wg_hbm.at[:, c], wgu.at[:, pl.ds(i * 256, 128)], in_sem.at[6 + 2 * i]))
        loads.append(pltpu.make_async_copy(wu_hbm.at[:, c], wgu.at[:, pl.ds(i * 256 + 128, 128)], in_sem.at[7 + 2 * i]))
    for cp in loads[:5]:
        cp.start()

    barrier = pltpu.get_barrier_semaphore()
    for p in peer:
        pl.semaphore_signal(barrier, inc=1, device_id={"tp": p}, device_id_type=MESH)
    pl.semaphore_wait(barrier, 2)

    def rows(d, j):
        return pl.ds(d * half + j * sub, sub)

    def span(d, j):
        return slice(d * half + j * sub, d * half + (j + 1) * sub)

    def message(d, j, m, src=None):
        slot = lax.rem(m, SLOTS)
        dst = slots.at[slot, rows(d, j)]
        return pltpu.make_async_remote_copy(
            src_ref=dst if src is None else src, dst_ref=dst,
            send_sem=send_sem.at[d, j, slot], recv_sem=recv_sem.at[d, j, slot],
            device_id={"tp": peer[d]}, device_id_type=MESH)

    def direct(d, j, phase):
        return pltpu.make_async_remote_copy(
            src_ref=stage.at[rows(d, j)], dst_ref=early.at[phase, pl.ds(j * sub, sub)],
            send_sem=early_send.at[phase, j], recv_sem=early_recv.at[phase, j],
            device_id={"tp": peer[1 - d]}, device_id_type=MESH)

    def when(cond, fn):
        if isinstance(cond, bool):
            if cond:
                fn()
        else:
            pl.when(cond)(fn)

    def take_credit(d, m):
        when(m >= SLOTS, lambda: pl.semaphore_wait(free_sem.at[d], 1))

    def give_credit(m):
        for d in range(2):
            when(m <= total_msgs - 1 - SLOTS, functools.partial(
                pl.semaphore_signal, free_sem.at[d], inc=1, device_id={"tp": peer[1 - d]}, device_id_type=MESH))

    tile = min(512, d_model // 2)

    tiles = d_model // tile

    def project(lhs, w, z, first, stop):
        @pl.loop(first, stop)
        def _(i):
            c = pl.ds(pl.multiple_of(i * tile, tile), tile)
            part[z, :, c] = jnp.dot(lhs(), w[:, c], preferred_element_type=F32)

    def reduce_start(phase, pieces):
        base = phase * (n - 1)
        for piece in pieces:
            piece(left, right, 1)
        stage[...] = part[1].astype(BF16)
        for j, d in pairs:
            if j == 0:
                take_credit(d, base)
            pl.when(leaves[d])(lambda d=d, j=j: direct(d, j, phase).start())
            pl.when(stays[d])(lambda d=d, j=j: message(d, j, base, stage.at[rows(d, j)]).start())

    def reduce_scatter(phase, pieces, finish):
        base = phase * (n - 1)
        for piece in pieces:
            piece(lax.rem(me + n - 2, n), lax.rem(me + 2, n), 0)

        @pl.loop(0, last)
        def _(s):
            m = base + s
            slot = lax.rem(m, SLOTS)
            z = lax.rem(s, 2)
            top, bottom = lax.rem(me + 2 * n - s - 3, n), lax.rem(me + s + 3, n)
            for j, d in pairs:
                ref = slots.at[slot, rows(d, j)]
                opens = jnp.logical_and(s == 0, stays[d])

                @pl.when(opens)
                def _():
                    ref[...] = part[z, span(d, j), :].astype(BF16)

                @pl.when(jnp.logical_not(opens))
                def _():
                    message(d, j, m).wait_recv()
                    ref[...] = (ref[...].astype(F32) + part[z, span(d, j), :]).astype(BF16)

                if j == 0:
                    take_credit(d, m + 1)
                message(d, j, m + 1, ref).start()
                if d == 1:
                    pieces[j](top, bottom, 1 - z)
            for j, d in pairs:
                handed = jnp.logical_and(s == 0, leaves[d])
                pl.when(handed)(lambda d=d, j=j: direct(d, j, phase).wait_send())
                pl.when(jnp.logical_not(handed))(lambda d=d, j=j: message(d, j, m).wait_send())
            pl.when(s >= 1)(lambda: give_credit(m - 1))

        m = base + last
        z = last % 2
        for j, d in pairs:
            message(d, j, m).wait_send()
        give_credit(m - 1)
        for j, d in pairs:
            @pl.when(stays[d])
            def _():
                direct(d, j, phase).wait_recv()
                part[z, span(d, j), :] = part[z, span(d, j), :] + early[phase, j * sub:(j + 1) * sub, :].astype(F32)
        for j, d in pairs:
            message(d, j, m).wait_recv()
            r = span(d, j)
            finish(r, slots[m % SLOTS, r, :].astype(F32) + part[z, r, :])
            if j == 0:
                take_credit(d, m + 1)
            message(d, j, m + 1, stage.at[rows(d, j)]).start()
            pl.when(leaves[d])(lambda d=d, j=j: direct(d, j, phase + 1).start())
        give_credit(m)

    def all_gather(phase, own, arrived, pieces, settle, then):
        base = phase * (n - 1)
        own()

        def work(j, m, s):
            if pieces:
                pieces[j](slots.at[lax.rem(m, SLOTS)], lax.rem(me + n - s - 1, n), lax.rem(me + s + 1, n))

        @pl.loop(0, last)
        def _(s):
            m = base + s
            slot = lax.rem(m, SLOTS)
            for j, d in pairs:
                message(d, j, m).wait_recv()
                if j == 0:
                    take_credit(d, m + 1)
                pl.when(jnp.logical_or(s < last - 1, stays[d]))(
                    lambda d=d, j=j: message(d, j, m + 1, slots.at[slot, rows(d, j)]).start())
                if d == 1:
                    pl.when(s >= 1)(lambda j=j: work(j, m - 1, s - 1))
            arrived(m, lax.rem(me + n - s - 1, n), lax.rem(me + s + 1, n))
            for j, d in pairs:
                message(d, j, m).wait_send()
                pl.when(jnp.logical_and(s == 0, leaves[d]))(lambda d=d, j=j: direct(d, j, phase).wait_send())

            @pl.when(s >= 1)
            def _():
                settle(m - 1)
                give_credit(m - 1)

        then()
        m = base + last
        for j in range(SUBS):
            work(j, m - 1, last - 1)
        for j, d in pairs:
            pl.when(stays[d])(lambda d=d, j=j: message(d, j, m).wait_send())
        settle(m - 1)
        give_credit(m - 1)
        for j, d in pairs:
            @pl.when(leaves[d])
            def _():
                message(d, j, m).wait_recv()

            @pl.when(stays[d])
            def _():
                direct(d, j, phase).wait_recv()
                slots[m % SLOTS, span(d, j), :] = early[phase, j * sub:(j + 1) * sub, :]
        arrived(m, right, left)
        for j in range(SUBS):
            work(j, m, last)
        settle(m)
        give_credit(m)

    kt = min(256, t_all)
    scale = HEAD ** -0.5
    lanes = kt // 128

    def attend_scores(top, bottom, z):
        r0 = pl.multiple_of(top * blk, half)
        r1 = pl.multiple_of(bottom * blk + half, half)
        qa, qb = q[pl.ds(r0, half), :], q[pl.ds(r1, half), :]
        qq = jnp.concatenate([t[:, h * HEAD:(h + 1) * HEAD] for t in (qa, qb) for h in range(heads)], axis=0)
        i = lax.broadcasted_iota(jnp.int32, (2 * heads * half, kt), 0)
        row = jnp.where(i < heads * half, r0, r1) + (i & (half - 1))
        ahead = row - lax.broadcasted_iota(jnp.int32, row.shape, 1)
        mx = None
        for b in range(t_all // kt):
            c = slice(b * kt, (b + 1) * kt)
            t = lax.dot_general(qq, k[c, :], (((1,), (1,)), ((), ())), preferred_element_type=F32) * scale
            t = jnp.where(ahead >= b * kt, t, -jnp.inf)
            sc[:, c] = t
            for y in range(lanes):
                g = t[:, y * 128:(y + 1) * 128]
                mx = g if mx is None else jnp.maximum(mx, g)
        top_score[...] = jnp.broadcast_to(jnp.max(mx, axis=-1, keepdims=True), mx.shape)

    def attend_values(top, bottom, z):
        mx = top_score[...]
        tot = None
        for b in range(t_all // 128):
            c = slice(b * 128, (b + 1) * 128)
            e = jnp.exp(sc[:, c] - mx)
            sc[:, c] = e
            tot = e if tot is None else tot + e
        rinv = 1.0 / jnp.sum(tot, axis=-1, keepdims=True)
        acc = None
        for b in range(t_all // kt):
            c = slice(b * kt, (b + 1) * kt)
            pr = (sc[:, c] * rinv).astype(BF16)
            g = jnp.dot(pr, v[c, :], preferred_element_type=F32)
            acc = g if acc is None else acc + g
        for y in range(2):
            for h in range(heads):
                w = y * heads + h
                orow[y * half:(y + 1) * half, h * HEAD:(h + 1) * HEAD] = acc[w * half:(w + 1) * half].astype(BF16)
        project(lambda: orow[...], wo, z, 0, tiles)

    output_pieces = (attend_scores, attend_values)

    for cp in loads[:5]:
        cp.wait()
    for cp in loads[5:]:
        cp.start()

    def finish_h(r, total):
        h = (hown[r, :].astype(F32) + total).astype(BF16)
        hown[r, :] = h
        h32 = h.astype(F32)
        inv = lax.rsqrt(jnp.mean(h32 * h32, axis=-1, keepdims=True) + EPS)
        stage[r, :] = (h32 * inv * g2_ref[...].astype(F32)).astype(BF16)

    reduce_start(0, output_pieces)
    reduce_scatter(0, output_pieces, finish_h)

    for cp in loads[5:]:
        cp.wait()

    def gate_up(first, stop, b_ref, top, bottom):
        @pl.loop(first, stop)
        def _(i):
            gu = jnp.dot(b_ref[...], wgu[:, pl.ds(pl.multiple_of(i * 256, 256), 256)], preferred_element_type=F32)
            g, up = gu[:, :128], gu[:, 128:]
            val = (jax.nn.silu(g) * up).astype(BF16)
            c = pl.ds(pl.multiple_of(i * 128, 128), 128)
            u[pl.ds(pl.multiple_of(top * blk, blk), half), c] = val[:half]
            u[pl.ds(pl.multiple_of(bottom * blk + half, half), half), c] = val[half:]

    def rows_of_u(top, bottom):
        return lambda: jnp.concatenate([u[pl.ds(pl.multiple_of(top * blk, blk), half), :],
                                        u[pl.ds(pl.multiple_of(bottom * blk + half, half), half), :]], axis=0)

    down_pieces = (lambda top, bottom, z: project(rows_of_u(top, bottom), wd, z, 0, tiles // 2),
                   lambda top, bottom, z: project(rows_of_u(top, bottom), wd, z, tiles // 2, tiles))
    cut = ff // 128 // 2

    all_gather(1, lambda: gate_up(0, ff // 128, stage, me, me), lambda m, top, bottom: None,
               (functools.partial(gate_up, 0, cut), functools.partial(gate_up, cut, ff // 128)),
               lambda m: None, lambda: reduce_start(2, down_pieces))

    def finish_y(r, total):
        stage[r, :] = (hown[r, :].astype(F32) + total).astype(BF16)

    reduce_scatter(2, down_pieces, finish_y)

    own = pltpu.make_async_copy(stage, y_hbm.at[pl.ds(pl.multiple_of(me * blk, blk), blk)], own_sem)

    def out(m, d, block):
        slot = lax.rem(m, SLOTS)
        return pltpu.make_async_copy(
            slots.at[slot, pl.ds(d * half, half)],
            y_hbm.at[pl.ds(pl.multiple_of(block * blk + d * half, half), half)], out_sem.at[d, slot])

    def arrived_y(m, top, bottom):
        out(m, 0, top).start()
        out(m, 1, bottom).start()

    def settle_y(m):
        for d in range(2):
            out(m, d, me).wait()

    all_gather(3, own.start, arrived_y, (), settle_y, lambda: None)
    own.wait()


def _ring(n, q, k, v, x, g2, wo, wg, wu, wd):
    t, d = x.shape
    ff = wd.shape[0]
    blk = t // n
    hbm = pl.BlockSpec(memory_space=pl.ANY)
    dma = pltpu.SemaphoreType.DMA
    return pl.pallas_call(
        functools.partial(_ring_kernel, n),
        out_shape=jax.ShapeDtypeStruct((t, d), BF16),
        in_specs=[hbm] * 4 + [pl.BlockSpec(memory_space=pltpu.VMEM)] + [hbm] * 4,
        out_specs=hbm,
        scratch_shapes=[
            pltpu.VMEM((SLOTS, blk, d), BF16),
            pltpu.VMEM((4, blk // 2, d), BF16),
            pltpu.VMEM((blk, d), BF16),
            pltpu.VMEM((2, blk, d), F32),
            pltpu.VMEM((blk, d), BF16),
            pltpu.VMEM((t, ff), BF16),
            pltpu.VMEM(q.shape, BF16),
            pltpu.VMEM(k.shape, BF16),
            pltpu.VMEM(v.shape, BF16),
            pltpu.VMEM((blk * (q.shape[1] // HEAD), t), F32),
            pltpu.VMEM((blk * (q.shape[1] // HEAD), 128), F32),
            pltpu.VMEM((blk, q.shape[1]), BF16),
            pltpu.VMEM(wo.shape, BF16),
            pltpu.VMEM((d, 2 * ff), BF16),
            pltpu.VMEM(wd.shape, BF16),
            dma((2, SUBS, SLOTS)),
            dma((2, SUBS, SLOTS)),
            dma((4, SUBS)),
            dma((4, SUBS)),
            dma((6 + 2 * (ff // 128),)),
            dma((2, SLOTS)),
            dma,
            pltpu.SemaphoreType.REGULAR((2,)),
        ],
        compiler_params=pltpu.CompilerParams(
            collective_id=0, has_side_effects=True, vmem_limit_bytes=60 << 20),
        name="ring_layer",
    )(q, k, v, x, g2, wo, wg, wu, wd)


def solution(mesh):
    tp = mesh.shape["tp"]

    def local(x, pos, g1, g2, wq, wk, wv, wo, wg, wu, wd):
        t, d = x.shape
        g = wk.shape[1] // HEAD
        r = lax.axis_index("tp")
        head = (r * g // tp).astype(jnp.int32).reshape(1)
        half = HEAD // 2
        inv = ROPE_BASE ** (-2.0 * jnp.arange(half, dtype=F32) / HEAD)
        ang = pos.astype(F32)[:, None] * inv
        c, s = jnp.cos(ang), jnp.sin(ang)
        cos = jnp.concatenate([c, c], axis=-1)
        sin = jnp.concatenate([-s, s], axis=-1)
        q, k, v = _qkv(head, x, g1.reshape(1, d), cos, sin, wq, wk, wv)
        y = _ring(tp, q, k, v, x, g2.reshape(1, d), wo, wg, wu, wd)
        return y, k.reshape(t, 1, HEAD), v.reshape(t, 1, HEAD)

    return jax.shard_map(
        local,
        mesh=mesh,
        in_specs=(P("dp", None), P("dp"), P(), P(), P(None, "tp"), P(), P(), P("tp", None),
                  P(None, "tp"), P(None, "tp"), P("tp", None)),
        out_specs=(P("dp", None), P("dp", "tp", None), P("dp", "tp", None)),
        check_vma=False,
    )
```

```python
import functools

import jax
import jax.numpy as jnp
from jax import lax
from jax.experimental import pallas as pl
from jax.experimental.pallas import tpu as pltpu
from jax.sharding import PartitionSpec as P

HEAD = 128
EPS = 1e-5
ROPE_BASE = 500000.0
SLOTS = 6
SUBS = 2
VMEM_RING = 50 * 10**6
MESH = pl.DeviceIdType.MESH
F32, BF16 = jnp.float32, jnp.bfloat16


def _qkv_kernel(hd_ref, x_ref, g1_ref, cos_ref, sin_ref, wq_ref, wk_ref, wv_ref,
                q_ref, k_ref, v_ref, wkv, a0, a1):
    i = pl.program_id(0)
    steps = pl.num_programs(0)
    hb, d = a0.shape
    hl = wq_ref.shape[1] // HEAD
    chunks = 4
    rows = hb // chunks
    kd = d // chunks

    def norm(x0, a, z):
        r = slice(x0 + z * rows, x0 + (z + 1) * rows)
        o = slice(z * rows, (z + 1) * rows)
        ss = None
        for t in range(d // 128):
            x32 = x_ref[r, t * 128:(t + 1) * 128].astype(F32)
            ss = x32 * x32 if ss is None else ss + x32 * x32
        inv = lax.rsqrt(jnp.sum(ss, axis=-1, keepdims=True) * (1.0 / d) + EPS)
        for t in range(d // 128):
            c = slice(t * 128, (t + 1) * 128)
            a[o, c] = (x_ref[r, c].astype(F32) * inv * g1_ref[:, c].astype(F32)).astype(BF16)

    def work(a, at, x0=None, into=None):
        kv = q = None
        for z in range(chunks):
            kk = slice(z * kd, (z + 1) * kd)
            t = jnp.dot(a[:, kk], wkv[kk, :], preferred_element_type=F32)
            kv = t if kv is None else kv + t
            t = jnp.dot(a[:, kk], wq_ref[kk, :], preferred_element_type=F32)
            q = t if q is None else q + t
            if into is not None:
                norm(x0, into, z)
        here = pl.ds(pl.multiple_of(at, hb), hb)
        c, s = cos_ref[here, :], sin_ref[here, :]

        def rope(t):
            return (t * c + pltpu.roll(t, HEAD // 2, 1) * s).astype(BF16)

        k_ref[here, :] = rope(kv[:, :HEAD])
        v_ref[here, :] = kv[:, HEAD:].astype(BF16)
        for h in range(hl):
            q_ref[here, h * HEAD:(h + 1) * HEAD] = rope(q[:, h * HEAD:(h + 1) * HEAD])

    @pl.when(i == 0)
    def _():
        wkv[:, :HEAD] = wk_ref[...]
        wkv[:, HEAD:] = wv_ref[...]
        for z in range(chunks):
            norm(0, a0, z)

    @pl.when(jnp.logical_and(i > 0, i < steps - 1))
    def _():
        work(a1, (2 * i - 1) * hb, 0, a0)

    @pl.when(i < steps - 1)
    def _():
        work(a0, 2 * i * hb, hb, a1)

    @pl.when(i == steps - 1)
    def _():
        work(a1, (2 * i - 1) * hb)


def _qkv(head, x, g1, cos, sin, wq, wk, wv):
    t, d = x.shape
    hb = min(t // 4, 256)
    nb = t // (2 * hb)
    hw = wq.shape[1]
    spec = pltpu.PrefetchScalarGridSpec(
        num_scalar_prefetch=1,
        grid=(nb + 1,),
        in_specs=[
            pl.BlockSpec((2 * hb, d), lambda i, hd: (jnp.minimum(i, nb - 1), 0)),
            pl.BlockSpec((1, d), lambda i, hd: (0, 0)),
            pl.BlockSpec((t, HEAD), lambda i, hd: (0, 0)),
            pl.BlockSpec((t, HEAD), lambda i, hd: (0, 0)),
            pl.BlockSpec((d, hw), lambda i, hd: (0, 0)),
            pl.BlockSpec((d, HEAD), lambda i, hd: (0, hd[0])),
            pl.BlockSpec((d, HEAD), lambda i, hd: (0, hd[0])),
        ],
        out_specs=[
            pl.BlockSpec((t, hw), lambda i, hd: (0, 0)),
            pl.BlockSpec((t, HEAD), lambda i, hd: (0, 0)),
            pl.BlockSpec((t, HEAD), lambda i, hd: (0, 0)),
        ],
        scratch_shapes=[
            pltpu.VMEM((d, 2 * HEAD), BF16),
            pltpu.VMEM((hb, d), BF16),
            pltpu.VMEM((hb, d), BF16),
        ],
    )
    return pl.pallas_call(
        _qkv_kernel,
        out_shape=(jax.ShapeDtypeStruct((t, hw), BF16), jax.ShapeDtypeStruct((t, HEAD), BF16),
                   jax.ShapeDtypeStruct((t, HEAD), BF16)),
        grid_spec=spec,
        compiler_params=pltpu.CompilerParams(
            dimension_semantics=("arbitrary",), vmem_limit_bytes=48 << 20),
        name="qkv",
    )(head, x, g1, cos, sin, wq, wk, wv)


def _ring_kernel(n, q_hbm, k_hbm, v_hbm, x_hbm, g2_ref, wo_hbm, wg_hbm, wu_hbm, wd_hbm, y,
                 slots, early, stage, part, hown, u, q, k, v, sc, top_score, orow, wo, wgu, wd,
                 send_sem, recv_sem, early_send, early_recv, in_sem, free_sem):
    me = lax.axis_index("tp")
    right, left = lax.rem(me + 1, n), lax.rem(me + n - 1, n)
    peer = (right, left)
    odd = lax.rem(me, 2)
    leaves = (odd == 1, odd == 0)
    stays = (odd == 0, odd == 1)
    d_model = wo.shape[1]
    ff = wd.shape[0]
    t_all = q.shape[0]
    heads = q.shape[1] // HEAD
    blk = stage.shape[0]
    half = blk // 2
    sub = half // SUBS
    last = n - 2
    total_msgs = 4 * (n - 1)
    pairs = [(j, d) for j in range(SUBS) for d in range(2)]

    loads = [pltpu.make_async_copy(src, dst, in_sem.at[i]) for i, (src, dst) in enumerate([
        (q_hbm, q), (k_hbm, k), (v_hbm, v), (wo_hbm, wo),
        (x_hbm.at[pl.ds(pl.multiple_of(me * blk, blk), blk)], hown), (wd_hbm, wd)])]
    for i in range(ff // 128):
        c = pl.ds(i * 128, 128)
        loads.append(pltpu.make_async_copy(wg_hbm.at[:, c], wgu.at[:, pl.ds(i * 256, 128)], in_sem.at[6 + 2 * i]))
        loads.append(pltpu.make_async_copy(wu_hbm.at[:, c], wgu.at[:, pl.ds(i * 256 + 128, 128)], in_sem.at[7 + 2 * i]))
    for cp in loads[:5]:
        cp.start()

    barrier = pltpu.get_barrier_semaphore()
    for p in peer:
        pl.semaphore_signal(barrier, inc=1, device_id={"tp": p}, device_id_type=MESH)
    pl.semaphore_wait(barrier, 2)

    def rows(d, j):
        return pl.ds(d * half + j * sub, sub)

    def span(d, j):
        return slice(d * half + j * sub, d * half + (j + 1) * sub)

    def message(d, j, m, src=None):
        slot = lax.rem(m, SLOTS)
        dst = slots.at[slot, rows(d, j)]
        return pltpu.make_async_remote_copy(
            src_ref=dst if src is None else src, dst_ref=dst,
            send_sem=send_sem.at[d, j, slot], recv_sem=recv_sem.at[d, j, slot],
            device_id={"tp": peer[d]}, device_id_type=MESH)

    def direct(d, j, phase):
        return pltpu.make_async_remote_copy(
            src_ref=stage.at[rows(d, j)], dst_ref=early.at[phase, pl.ds(j * sub, sub)],
            send_sem=early_send.at[phase, j], recv_sem=early_recv.at[phase, j],
            device_id={"tp": peer[1 - d]}, device_id_type=MESH)

    def when(cond, fn):
        if isinstance(cond, bool):
            if cond:
                fn()
        else:
            pl.when(cond)(fn)

    def take_credit(d, m):
        when(m >= SLOTS, lambda: pl.semaphore_wait(free_sem.at[d], 1))

    def give_credit(m):
        for d in range(2):
            when(m <= total_msgs - 1 - SLOTS, functools.partial(
                pl.semaphore_signal, free_sem.at[d], inc=1, device_id={"tp": peer[1 - d]}, device_id_type=MESH))

    tile = min(512, d_model // 2)

    tiles = d_model // tile

    def project(lhs, w, z, first, stop):
        @pl.loop(first, stop)
        def _(i):
            c = pl.ds(pl.multiple_of(i * tile, tile), tile)
            part[z, :, c] = jnp.dot(lhs(), w[:, c], preferred_element_type=F32)

    def reduce_start(phase, pieces):
        base = phase * (n - 1)
        for piece in pieces:
            piece(left, right, 1)
        stage[...] = part[1].astype(BF16)
        for j, d in pairs:
            if j == 0:
                take_credit(d, base)
            pl.when(leaves[d])(lambda d=d, j=j: direct(d, j, phase).start())
            pl.when(stays[d])(lambda d=d, j=j: message(d, j, base, stage.at[rows(d, j)]).start())
        for piece in pieces:
            piece(lax.rem(me + n - 2, n), lax.rem(me + 2, n), 0)

    def reduce_scatter(phase, pieces, finish, begin=None, extra=None, end=None):
        base = phase * (n - 1)

        @pl.loop(0, last)
        def _(s):
            m = base + s
            slot = lax.rem(m, SLOTS)
            z = lax.rem(s, 2)
            top, bottom = lax.rem(me + 2 * n - s - 3, n), lax.rem(me + s + 3, n)
            if begin is not None:
                begin(s)
            for j, d in pairs:
                ref = slots.at[slot, rows(d, j)]
                opens = jnp.logical_and(s == 0, stays[d])

                @pl.when(opens)
                def _():
                    ref[...] = part[z, span(d, j), :].astype(BF16)

                @pl.when(jnp.logical_not(opens))
                def _():
                    message(d, j, m).wait_recv()
                    ref[...] = (ref[...].astype(F32) + part[z, span(d, j), :]).astype(BF16)

                if j == 0:
                    take_credit(d, m + 1)
                message(d, j, m + 1, ref).start()
                if d == 1:
                    pieces[j](top, bottom, 1 - z)
                    if extra is not None:
                        extra(s, j)
            for j, d in pairs:
                handed = jnp.logical_and(s == 0, leaves[d])
                pl.when(handed)(lambda d=d, j=j: direct(d, j, phase).wait_send())
                pl.when(jnp.logical_not(handed))(lambda d=d, j=j: message(d, j, m).wait_send())
            if end is not None:
                end(s)
            pl.when(s >= 1)(lambda: give_credit(m - 1))

        m = base + last
        z = last % 2
        for j, d in pairs:
            @pl.when(stays[d])
            def _():
                direct(d, j, phase).wait_recv()
                part[z, span(d, j), :] = part[z, span(d, j), :] + early[phase, j * sub:(j + 1) * sub, :].astype(F32)
        for j, d in pairs:
            message(d, j, m).wait_recv()
            r = span(d, j)
            finish(r, slots[m % SLOTS, r, :].astype(F32) + part[z, r, :])
            if j == 0:
                take_credit(d, m + 1)
            message(d, j, m + 1, stage.at[rows(d, j)]).start()
            pl.when(leaves[d])(lambda d=d, j=j: direct(d, j, phase + 1).start())
        for j, d in pairs:
            message(d, j, m).wait_send()
        give_credit(m - 1)
        give_credit(m)

    def last_arrival(d, j, phase):
        m = phase * (n - 1) + last

        @pl.when(leaves[d])
        def _():
            message(d, j, m).wait_recv()

        @pl.when(stays[d])
        def _():
            direct(d, j, phase).wait_recv()
            slots[m % SLOTS, span(d, j), :] = early[phase, j * sub:(j + 1) * sub, :]

    def all_gather(phase, own, arrived, stop):
        base = phase * (n - 1)
        own()

        @pl.loop(0, stop)
        def _(s):
            m = base + s
            slot = lax.rem(m, SLOTS)
            for j, d in pairs:
                message(d, j, m).wait_recv()
                if j == 0:
                    take_credit(d, m + 1)
                onward = functools.partial(lambda d, j: message(d, j, m + 1, slots.at[slot, rows(d, j)]).start(), d, j)
                if stop < last:
                    onward()
                else:
                    pl.when(jnp.logical_or(s < last - 1, stays[d]))(onward)
                if d == 1:
                    arrived(j, s)
            for j, d in pairs:
                message(d, j, m).wait_send()
                pl.when(jnp.logical_and(s == 0, leaves[d]))(lambda d=d, j=j: direct(d, j, phase).wait_send())
            pl.when(s >= 1)(lambda: give_credit(m - 1))

    kt = min(256, t_all)
    scale = HEAD ** -0.5
    lanes = kt // 128

    def attend_scores(top, bottom, z):
        r0 = pl.multiple_of(top * blk, half)
        r1 = pl.multiple_of(bottom * blk + half, half)
        qa, qb = q[pl.ds(r0, half), :], q[pl.ds(r1, half), :]
        qq = jnp.concatenate([t[:, h * HEAD:(h + 1) * HEAD] for t in (qa, qb) for h in range(heads)], axis=0)
        i = lax.broadcasted_iota(jnp.int32, (2 * heads * half, kt), 0)
        row = jnp.where(i < heads * half, r0, r1) + (i & (half - 1))
        ahead = row - lax.broadcasted_iota(jnp.int32, row.shape, 1)
        mx = None
        for b in range(t_all // kt):
            c = slice(b * kt, (b + 1) * kt)
            t = lax.dot_general(qq, k[c, :], (((1,), (1,)), ((), ())), preferred_element_type=F32) * scale
            t = jnp.where(ahead >= b * kt, t, -jnp.inf)
            sc[:, c] = t
            for y in range(lanes):
                g = t[:, y * 128:(y + 1) * 128]
                mx = g if mx is None else jnp.maximum(mx, g)
        top_score[...] = jnp.broadcast_to(jnp.max(mx, axis=-1, keepdims=True), mx.shape)

    def attend_values(top, bottom, z):
        mx = top_score[...]
        tot = None
        for b in range(t_all // 128):
            c = slice(b * 128, (b + 1) * 128)
            e = jnp.exp(sc[:, c] - mx)
            sc[:, c] = e
            tot = e if tot is None else tot + e
        rinv = 1.0 / jnp.sum(tot, axis=-1, keepdims=True)
        acc = None
        for b in range(t_all // kt):
            c = slice(b * kt, (b + 1) * kt)
            pr = (sc[:, c] * rinv).astype(BF16)
            g = jnp.dot(pr, v[c, :], preferred_element_type=F32)
            acc = g if acc is None else acc + g
        for y in range(2):
            for h in range(heads):
                w = y * heads + h
                orow[y * half:(y + 1) * half, h * HEAD:(h + 1) * HEAD] = acc[w * half:(w + 1) * half].astype(BF16)
        project(lambda: orow[...], wo, z, 0, tiles)

    output_pieces = (attend_scores, attend_values)

    for cp in loads[:5]:
        cp.wait()
    for cp in loads[5:]:
        cp.start()

    def finish_h(r, total):
        h = (hown[r, :].astype(F32) + total).astype(BF16)
        hown[r, :] = h
        h32 = h.astype(F32)
        inv = lax.rsqrt(jnp.mean(h32 * h32, axis=-1, keepdims=True) + EPS)
        stage[r, :] = (h32 * inv * g2_ref[...].astype(F32)).astype(BF16)

    reduce_start(0, output_pieces)
    reduce_scatter(0, output_pieces, finish_h)

    for cp in loads[5:]:
        cp.wait()

    def gate_up(first, stop, b_ref, top, bottom):
        @pl.loop(first, stop)
        def _(i):
            gu = jnp.dot(b_ref[...], wgu[:, pl.ds(pl.multiple_of(i * 256, 256), 256)], preferred_element_type=F32)
            g, up = gu[:, :128], gu[:, 128:]
            val = (jax.nn.silu(g) * up).astype(BF16)
            c = pl.ds(pl.multiple_of(i * 128, 128), 128)
            u[pl.ds(pl.multiple_of(top * blk, blk), half), c] = val[:half]
            u[pl.ds(pl.multiple_of(bottom * blk + half, half), half), c] = val[half:]

    def rows_of_u(top, bottom):
        return lambda: jnp.concatenate([u[pl.ds(pl.multiple_of(top * blk, blk), half), :],
                                        u[pl.ds(pl.multiple_of(bottom * blk + half, half), half), :]], axis=0)

    down_pieces = (lambda top, bottom, z: project(rows_of_u(top, bottom), wd, z, 0, tiles // 2),
                   lambda top, bottom, z: project(rows_of_u(top, bottom), wd, z, tiles // 2, tiles))
    cut = ff // 128 // 2

    first = n - 1
    halves = ((0, cut), (cut, ff // 128))

    def gate_up_of(j, s):
        gate_up(*halves[j], slots.at[lax.rem(first + s, SLOTS)], lax.rem(me + n - s - 1, n), lax.rem(me + s + 1, n))

    all_gather(1, lambda: gate_up(0, ff // 128, stage, me, me),
               lambda j, s: pl.when(s >= 1)(lambda: gate_up_of(j, s - 1)), last - 1)

    for d in range(2):
        take_credit(d, first + last)
    reduce_start(2, down_pieces)
    m13, m14 = first + last - 1, first + last
    for j, d in pairs:
        message(d, j, m13).wait_recv()
        pl.when(stays[d])(lambda d=d, j=j: message(d, j, m14, slots.at[m13 % SLOTS, rows(d, j)]).start())
        if d == 1:
            gate_up_of(j, last - 2)

    def begin(s):
        @pl.when(s == 1)
        def _():
            for j, d in pairs:
                last_arrival(d, j, 1)

    def extra(s, j):
        pl.when(s == 0)(lambda: gate_up_of(j, last - 1))
        pl.when(s == 1)(lambda: gate_up_of(j, last))

    def end(s):
        @pl.when(s == 0)
        def _():
            for j, d in pairs:
                message(d, j, m13).wait_send()
            give_credit(m13 - 1)
            for j, d in pairs:
                pl.when(stays[d])(lambda d=d, j=j: message(d, j, m14).wait_send())
            give_credit(m13)

        @pl.when(s == 1)
        def _():
            give_credit(m14)

    def finish_y(r, total):
        stage[r, :] = (hown[r, :].astype(F32) + total).astype(BF16)

    reduce_scatter(2, down_pieces, finish_y, begin, extra, end)

    def own():
        y[pl.ds(pl.multiple_of(me * blk, blk), blk), :] = stage[...]

    def store(j, slot, top, bottom):
        for d, block in enumerate((top, bottom)):
            at = pl.multiple_of(block * blk + d * half + j * sub, sub)
            y[pl.ds(at, sub), :] = slots[slot, span(d, j), :]

    base = 3 * (n - 1)
    all_gather(3, own, lambda j, s: store(j, lax.rem(base + s, SLOTS), lax.rem(me + n - s - 1, n),
                                          lax.rem(me + s + 1, n)), last)
    m = base + last
    for j, d in pairs:
        last_arrival(d, j, 3)
        if d == 1:
            store(j, m % SLOTS, right, left)
    for j, d in pairs:
        pl.when(stays[d])(lambda d=d, j=j: message(d, j, m).wait_send())
    give_credit(m - 1)
    give_credit(m)


def _ring(n, q, k, v, x, g2, wo, wg, wu, wd):
    t, d = x.shape
    ff = wd.shape[0]
    blk = t // n
    hbm = pl.BlockSpec(memory_space=pl.ANY)
    dma = pltpu.SemaphoreType.DMA
    return pl.pallas_call(
        functools.partial(_ring_kernel, n),
        out_shape=pltpu.VMEM((t, d), BF16),
        in_specs=[hbm] * 4 + [pl.BlockSpec(memory_space=pltpu.VMEM)] + [hbm] * 4,
        out_specs=pl.BlockSpec(memory_space=pltpu.VMEM),
        scratch_shapes=[
            pltpu.VMEM((SLOTS, blk, d), BF16),
            pltpu.VMEM((4, blk // 2, d), BF16),
            pltpu.VMEM((blk, d), BF16),
            pltpu.VMEM((2, blk, d), F32),
            pltpu.VMEM((blk, d), BF16),
            pltpu.VMEM((t, ff), BF16),
            pltpu.VMEM(q.shape, BF16),
            pltpu.VMEM(k.shape, BF16),
            pltpu.VMEM(v.shape, BF16),
            pltpu.VMEM((blk * (q.shape[1] // HEAD), t), F32),
            pltpu.VMEM((blk * (q.shape[1] // HEAD), 128), F32),
            pltpu.VMEM((blk, q.shape[1]), BF16),
            pltpu.VMEM(wo.shape, BF16),
            pltpu.VMEM((d, 2 * ff), BF16),
            pltpu.VMEM(wd.shape, BF16),
            dma((2, SUBS, SLOTS)),
            dma((2, SUBS, SLOTS)),
            dma((4, SUBS)),
            dma((4, SUBS)),
            dma((6 + 2 * (ff // 128),)),
            pltpu.SemaphoreType.REGULAR((2,)),
        ],
        compiler_params=pltpu.CompilerParams(
            collective_id=0, has_side_effects=True, vmem_limit_bytes=VMEM_RING),
        name="ring_layer",
    )(q, k, v, x, g2, wo, wg, wu, wd)


def _store_kernel(y_vmem, y_hbm, sem):
    parts = 8
    r = y_vmem.shape[0] // parts
    copies = [pltpu.make_async_copy(y_vmem.at[pl.ds(i * r, r)], y_hbm.at[pl.ds(i * r, r)], sem.at[i])
              for i in range(parts)]
    for cp in copies:
        cp.start()
    for cp in copies:
        cp.wait()


def _store(y):
    return pl.pallas_call(
        _store_kernel,
        out_shape=jax.ShapeDtypeStruct(y.shape, y.dtype),
        in_specs=[pl.BlockSpec(memory_space=pltpu.VMEM)],
        out_specs=pl.BlockSpec(memory_space=pl.ANY),
        scratch_shapes=[pltpu.SemaphoreType.DMA((8,))],
        compiler_params=pltpu.CompilerParams(vmem_limit_bytes=4 << 20),
        name="store",
    )(y)


def solution(mesh):
    tp = mesh.shape["tp"]

    def local(x, pos, g1, g2, wq, wk, wv, wo, wg, wu, wd):
        t, d = x.shape
        g = wk.shape[1] // HEAD
        r = lax.axis_index("tp")
        head = (r * g // tp).astype(jnp.int32).reshape(1)
        half = HEAD // 2
        inv = ROPE_BASE ** (-2.0 * jnp.arange(half, dtype=F32) / HEAD)
        ang = pos.astype(F32)[:, None] * inv
        c, s = jnp.cos(ang), jnp.sin(ang)
        cos = jnp.concatenate([c, c], axis=-1)
        sin = jnp.concatenate([-s, s], axis=-1)
        q, k, v = _qkv(head, x, g1.reshape(1, d), cos, sin, wq, wk, wv)
        y = _store(_ring(tp, q, k, v, x, g2.reshape(1, d), wo, wg, wu, wd))
        return y, k.reshape(t, 1, HEAD), v.reshape(t, 1, HEAD)

    return jax.shard_map(
        local,
        mesh=mesh,
        in_specs=(P("dp", None), P("dp"), P(), P(), P(None, "tp"), P(), P(), P("tp", None),
                  P(None, "tp"), P(None, "tp"), P("tp", None)),
        out_specs=(P("dp", None), P("dp", "tp", None), P("dp", "tp", None)),
        check_vma=False,
    )
```

```python
import functools

import jax
import jax.numpy as jnp
from jax import lax
from jax.experimental import pallas as pl
from jax.experimental.pallas import tpu as pltpu
from jax.sharding import PartitionSpec as P

HEAD = 128
EPS = 1e-5
ROPE_BASE = 500000.0
SLOTS = 6
SUBS = 2
VMEM_RING = 50 * 10**6
MESH = pl.DeviceIdType.MESH
F32, BF16 = jnp.float32, jnp.bfloat16


def _qkv_kernel(hd_ref, x_ref, g1_ref, cos_ref, sin_ref, wq_ref, wk_ref, wv_ref,
                q_ref, k_ref, v_ref, wkv, a0, a1):
    i = pl.program_id(0)
    steps = pl.num_programs(0)
    hb, d = a0.shape
    hl = wq_ref.shape[1] // HEAD
    chunks = 4
    rows = hb // chunks
    kd = d // chunks

    def norm(x0, a, z):
        r = slice(x0 + z * rows, x0 + (z + 1) * rows)
        o = slice(z * rows, (z + 1) * rows)
        ss = None
        for t in range(d // 128):
            x32 = x_ref[r, t * 128:(t + 1) * 128].astype(F32)
            ss = x32 * x32 if ss is None else ss + x32 * x32
        inv = lax.rsqrt(jnp.sum(ss, axis=-1, keepdims=True) * (1.0 / d) + EPS)
        for t in range(d // 128):
            c = slice(t * 128, (t + 1) * 128)
            a[o, c] = (x_ref[r, c].astype(F32) * inv * g1_ref[:, c].astype(F32)).astype(BF16)

    def work(a, at, x0=None, into=None):
        kv = q = None
        for z in range(chunks):
            kk = slice(z * kd, (z + 1) * kd)
            t = jnp.dot(a[:, kk], wkv[kk, :], preferred_element_type=F32)
            kv = t if kv is None else kv + t
            t = jnp.dot(a[:, kk], wq_ref[kk, :], preferred_element_type=F32)
            q = t if q is None else q + t
            if into is not None:
                norm(x0, into, z)
        here = pl.ds(pl.multiple_of(at, hb), hb)
        c, s = cos_ref[here, :], sin_ref[here, :]

        def rope(t):
            return (t * c + pltpu.roll(t, HEAD // 2, 1) * s).astype(BF16)

        k_ref[here, :] = rope(kv[:, :HEAD])
        v_ref[here, :] = kv[:, HEAD:].astype(BF16)
        for h in range(hl):
            q_ref[here, h * HEAD:(h + 1) * HEAD] = rope(q[:, h * HEAD:(h + 1) * HEAD])

    @pl.when(i == 0)
    def _():
        wkv[:, :HEAD] = wk_ref[...]
        wkv[:, HEAD:] = wv_ref[...]
        for z in range(chunks):
            norm(0, a0, z)

    @pl.when(jnp.logical_and(i > 0, i < steps - 1))
    def _():
        work(a1, (2 * i - 1) * hb, 0, a0)

    @pl.when(i < steps - 1)
    def _():
        work(a0, 2 * i * hb, hb, a1)

    @pl.when(i == steps - 1)
    def _():
        work(a1, (2 * i - 1) * hb)


def _qkv(head, x, g1, cos, sin, wq, wk, wv):
    t, d = x.shape
    hb = min(t // 4, 256)
    nb = t // (2 * hb)
    hw = wq.shape[1]
    spec = pltpu.PrefetchScalarGridSpec(
        num_scalar_prefetch=1,
        grid=(nb + 1,),
        in_specs=[
            pl.BlockSpec((2 * hb, d), lambda i, hd: (jnp.minimum(i, nb - 1), 0)),
            pl.BlockSpec((1, d), lambda i, hd: (0, 0)),
            pl.BlockSpec((t, HEAD), lambda i, hd: (0, 0)),
            pl.BlockSpec((t, HEAD), lambda i, hd: (0, 0)),
            pl.BlockSpec((d, hw), lambda i, hd: (0, 0)),
            pl.BlockSpec((d, HEAD), lambda i, hd: (0, hd[0])),
            pl.BlockSpec((d, HEAD), lambda i, hd: (0, hd[0])),
        ],
        out_specs=[
            pl.BlockSpec((t, hw), lambda i, hd: (0, 0)),
            pl.BlockSpec((t, HEAD), lambda i, hd: (0, 0)),
            pl.BlockSpec((t, HEAD), lambda i, hd: (0, 0)),
        ],
        scratch_shapes=[
            pltpu.VMEM((d, 2 * HEAD), BF16),
            pltpu.VMEM((hb, d), BF16),
            pltpu.VMEM((hb, d), BF16),
        ],
    )
    return pl.pallas_call(
        _qkv_kernel,
        out_shape=(jax.ShapeDtypeStruct((t, hw), BF16), jax.ShapeDtypeStruct((t, HEAD), BF16),
                   jax.ShapeDtypeStruct((t, HEAD), BF16)),
        grid_spec=spec,
        compiler_params=pltpu.CompilerParams(
            dimension_semantics=("arbitrary",), vmem_limit_bytes=48 << 20),
        name="qkv",
    )(head, x, g1, cos, sin, wq, wk, wv)


def _ring_kernel(n, q_hbm, k_hbm, v_hbm, x_hbm, g2_ref, wo_hbm, wg_hbm, wu_hbm, wd_hbm, y,
                 slots, early, stage, part, hown, u, q, k, v, sc, top_score, orow, wo, wgu, wd,
                 send_sem, recv_sem, early_send, early_recv, in_sem, free_sem):
    me = lax.axis_index("tp")
    right, left = lax.rem(me + 1, n), lax.rem(me + n - 1, n)
    peer = (right, left)
    odd = lax.rem(me, 2)
    leaves = (odd == 1, odd == 0)
    stays = (odd == 0, odd == 1)
    d_model = wo.shape[1]
    ff = wd.shape[0]
    t_all = q.shape[0]
    heads = q.shape[1] // HEAD
    blk = stage.shape[0]
    half = blk // 2
    sub = half // SUBS
    last = n - 2
    total_msgs = 4 * (n - 1)
    pairs = [(j, d) for j in range(SUBS) for d in range(2)]

    loads = [pltpu.make_async_copy(src, dst, in_sem.at[i]) for i, (src, dst) in enumerate([
        (q_hbm, q), (k_hbm, k), (v_hbm, v), (wo_hbm, wo),
        (x_hbm.at[pl.ds(pl.multiple_of(me * blk, blk), blk)], hown), (wd_hbm, wd)])]
    for i in range(ff // 128):
        c = pl.ds(i * 128, 128)
        loads.append(pltpu.make_async_copy(wg_hbm.at[:, c], wgu.at[:, pl.ds(i * 256, 128)], in_sem.at[6 + 2 * i]))
        loads.append(pltpu.make_async_copy(wu_hbm.at[:, c], wgu.at[:, pl.ds(i * 256 + 128, 128)], in_sem.at[7 + 2 * i]))
    for cp in loads[:5]:
        cp.start()

    barrier = pltpu.get_barrier_semaphore()
    for p in peer:
        pl.semaphore_signal(barrier, inc=1, device_id={"tp": p}, device_id_type=MESH)

    def rows(d, j):
        return pl.ds(d * half + j * sub, sub)

    def span(d, j):
        return slice(d * half + j * sub, d * half + (j + 1) * sub)

    def message(d, j, m, src=None):
        slot = lax.rem(m, SLOTS)
        dst = slots.at[slot, rows(d, j)]
        return pltpu.make_async_remote_copy(
            src_ref=dst if src is None else src, dst_ref=dst,
            send_sem=send_sem.at[d, j, slot], recv_sem=recv_sem.at[d, j, slot],
            device_id={"tp": peer[d]}, device_id_type=MESH)

    def direct(d, j, phase):
        return pltpu.make_async_remote_copy(
            src_ref=stage.at[rows(d, j)], dst_ref=early.at[phase, pl.ds(j * sub, sub)],
            send_sem=early_send.at[phase, j], recv_sem=early_recv.at[phase, j],
            device_id={"tp": peer[1 - d]}, device_id_type=MESH)

    def when(cond, fn):
        if isinstance(cond, bool):
            if cond:
                fn()
        else:
            pl.when(cond)(fn)

    def take_credit(d, m):
        when(m >= SLOTS, lambda: pl.semaphore_wait(free_sem.at[d], 1))

    def give_credit(m):
        for d in range(2):
            when(m <= total_msgs - 1 - SLOTS, functools.partial(
                pl.semaphore_signal, free_sem.at[d], inc=1, device_id={"tp": peer[1 - d]}, device_id_type=MESH))

    tile = min(512, d_model // 2)

    tiles = d_model // tile

    def project(lhs, w, z, first, stop):
        @pl.loop(first, stop)
        def _(i):
            c = pl.ds(pl.multiple_of(i * tile, tile), tile)
            part[z, :, c] = jnp.dot(lhs(), w[:, c], preferred_element_type=F32)

    def reduce_start(phase, pieces):
        base = phase * (n - 1)
        for piece in pieces:
            piece(left, right, 1)
        stage[...] = part[1].astype(BF16)
        for j, d in pairs:
            if j == 0:
                take_credit(d, base)
            pl.when(leaves[d])(lambda d=d, j=j: direct(d, j, phase).start())
            pl.when(stays[d])(lambda d=d, j=j: message(d, j, base, stage.at[rows(d, j)]).start())
        for piece in pieces:
            piece(lax.rem(me + n - 2, n), lax.rem(me + 2, n), 0)

    def forward(d, j, m, ref):
        if j == 0:
            take_credit(d, m)
        message(d, j, m, ref).start()

    def add_and_forward(d, j, m, z):
        message(d, j, m).wait_recv()
        ref = slots.at[lax.rem(m, SLOTS), rows(d, j)]
        ref[...] = (ref[...].astype(F32) + part[z, span(d, j), :]).astype(BF16)
        forward(d, j, m + 1, ref)

    def reduce_scatter(phase, pieces, finish, begin=None, extra=None, end=None):
        base = phase * (n - 1)

        @pl.loop(0, last)
        def _(s):
            m = base + s
            slot = lax.rem(m, SLOTS)
            z = lax.rem(s, 2)
            top, bottom = lax.rem(me + 2 * n - s - 3, n), lax.rem(me + s + 3, n)
            if begin is not None:
                begin(s)
            for j, d in pairs:
                ref = slots.at[slot, rows(d, j)]
                opens = jnp.logical_and(s == 0, stays[d])

                @pl.when(opens)
                def _():
                    ref[...] = part[z, span(d, j), :].astype(BF16)

                @pl.when(s >= 1 if phase == 0 else jnp.logical_not(opens))
                def _():
                    add_and_forward(d, j, m, z)

                @pl.when(opens)
                def _():
                    forward(d, j, m + 1, ref)
                if d == 1:
                    pieces[j](top, bottom, 1 - z)
                    if extra is not None:
                        extra(s, j)
            for j, d in pairs:
                handed = jnp.logical_and(s == 0, leaves[d])
                pl.when(handed)(lambda d=d, j=j: direct(d, j, phase).wait_send())
                pl.when(jnp.logical_not(handed))(lambda d=d, j=j: message(d, j, m).wait_send())
            if end is not None:
                end(s)
            pl.when(s >= 1)(lambda: give_credit(m - 1))

        m = base + last
        z = last % 2
        for j, d in pairs:
            @pl.when(stays[d])
            def _():
                direct(d, j, phase).wait_recv()
                part[z, span(d, j), :] = part[z, span(d, j), :] + early[phase, j * sub:(j + 1) * sub, :].astype(F32)
        for j, d in pairs:
            message(d, j, m).wait_recv()
            r = span(d, j)
            finish(r, slots[m % SLOTS, r, :].astype(F32) + part[z, r, :])
            if j == 0:
                take_credit(d, m + 1)
            message(d, j, m + 1, stage.at[rows(d, j)]).start()
            pl.when(leaves[d])(lambda d=d, j=j: direct(d, j, phase + 1).start())
        for j, d in pairs:
            message(d, j, m).wait_send()
        give_credit(m - 1)
        give_credit(m)

    def last_arrival(d, j, phase):
        m = phase * (n - 1) + last

        @pl.when(leaves[d])
        def _():
            message(d, j, m).wait_recv()

        @pl.when(stays[d])
        def _():
            direct(d, j, phase).wait_recv()
            slots[m % SLOTS, span(d, j), :] = early[phase, j * sub:(j + 1) * sub, :]

    def all_gather(phase, own, arrived, stop):
        base = phase * (n - 1)
        own()

        @pl.loop(0, stop)
        def _(s):
            m = base + s
            slot = lax.rem(m, SLOTS)
            for j, d in pairs:
                message(d, j, m).wait_recv()
                if j == 0:
                    take_credit(d, m + 1)
                onward = functools.partial(lambda d, j: message(d, j, m + 1, slots.at[slot, rows(d, j)]).start(), d, j)
                if stop < last:
                    onward()
                else:
                    pl.when(jnp.logical_or(s < last - 1, stays[d]))(onward)
                if d == 1:
                    arrived(j, s)
            for j, d in pairs:
                message(d, j, m).wait_send()
                pl.when(jnp.logical_and(s == 0, leaves[d]))(lambda d=d, j=j: direct(d, j, phase).wait_send())
            pl.when(s >= 1)(lambda: give_credit(m - 1))

    kt = min(256, t_all)
    scale = HEAD ** -0.5
    lanes = kt // 128

    def attend_scores(top, bottom, z):
        r0 = pl.multiple_of(top * blk, half)
        r1 = pl.multiple_of(bottom * blk + half, half)
        qa, qb = q[pl.ds(r0, half), :], q[pl.ds(r1, half), :]
        qq = jnp.concatenate([t[:, h * HEAD:(h + 1) * HEAD] for t in (qa, qb) for h in range(heads)], axis=0)
        i = lax.broadcasted_iota(jnp.int32, (2 * heads * half, kt), 0)
        row = jnp.where(i < heads * half, r0, r1) + (i & (half - 1))
        ahead = row - lax.broadcasted_iota(jnp.int32, row.shape, 1)
        mx = None
        for b in range(t_all // kt):
            c = slice(b * kt, (b + 1) * kt)
            t = lax.dot_general(qq, k[c, :], (((1,), (1,)), ((), ())), preferred_element_type=F32) * scale
            t = jnp.where(ahead >= b * kt, t, -jnp.inf)
            sc[:, c] = t
            for y in range(lanes):
                g = t[:, y * 128:(y + 1) * 128]
                mx = g if mx is None else jnp.maximum(mx, g)
        top_score[...] = jnp.broadcast_to(jnp.max(mx, axis=-1, keepdims=True), mx.shape)

    def attend_values(top, bottom, z):
        mx = top_score[...]
        tot = None
        for b in range(t_all // 128):
            c = slice(b * 128, (b + 1) * 128)
            e = jnp.exp(sc[:, c] - mx)
            sc[:, c] = e
            tot = e if tot is None else tot + e
        rinv = 1.0 / jnp.sum(tot, axis=-1, keepdims=True)
        acc = None
        for b in range(t_all // kt):
            c = slice(b * kt, (b + 1) * kt)
            pr = (sc[:, c] * rinv).astype(BF16)
            g = jnp.dot(pr, v[c, :], preferred_element_type=F32)
            acc = g if acc is None else acc + g
        for y in range(2):
            for h in range(heads):
                w = y * heads + h
                orow[y * half:(y + 1) * half, h * HEAD:(h + 1) * HEAD] = acc[w * half:(w + 1) * half].astype(BF16)
        project(lambda: orow[...], wo, z, 0, tiles)

    output_pieces = (attend_scores, attend_values)


    def finish_h(r, total):
        h = (hown[r, :].astype(F32) + total).astype(BF16)
        hown[r, :] = h
        h32 = h.astype(F32)
        inv = lax.rsqrt(jnp.mean(h32 * h32, axis=-1, keepdims=True) + EPS)
        stage[r, :] = (h32 * inv * g2_ref[...].astype(F32)).astype(BF16)

    def by_parity(a, b):
        return lax.rem(jnp.where(odd == 1, a, b), n)

    def cast_to_stage(d, z):
        for j in range(SUBS):
            stage[rows(d, j), :] = part[z, span(d, j), :].astype(BF16)

    top, bottom = by_parity(me + n - 2, me + n - 1), by_parity(me + 1, me + 2)
    for cp in loads[:2]:
        cp.wait()
    attend_scores(top, bottom, 0)
    for cp in loads[2:4]:
        cp.wait()
    for cp in loads[5:]:
        cp.start()
    attend_values(top, bottom, 0)
    pl.semaphore_wait(barrier, 2)
    for d in range(2):
        @pl.when(stays[d])
        def _():
            cast_to_stage(d, 0)
            for j in range(SUBS):
                message(d, j, 0, stage.at[rows(d, j)]).start()
    for d in range(2):
        @pl.when(leaves[d])
        def _():
            for j in range(SUBS):
                add_and_forward(d, j, 0, 0)
    top, bottom = by_parity(me + n - 1, me + n - 2), by_parity(me + 2, me + 1)
    attend_scores(top, bottom, 1)
    attend_values(top, bottom, 1)
    for d in range(2):
        @pl.when(leaves[d])
        def _():
            cast_to_stage(d, 1)
            for j in range(SUBS):
                direct(d, j, 0).start()

        @pl.when(stays[d])
        def _():
            for j in range(SUBS):
                part[0, span(d, j), :] = part[1, span(d, j), :]
    loads[4].wait()
    reduce_scatter(0, output_pieces, finish_h)

    for cp in loads[5:]:
        cp.wait()

    def gate_up(first, stop, b_ref, top, bottom):
        @pl.loop(first, stop)
        def _(i):
            gu = jnp.dot(b_ref[...], wgu[:, pl.ds(pl.multiple_of(i * 256, 256), 256)], preferred_element_type=F32)
            g, up = gu[:, :128], gu[:, 128:]
            val = (jax.nn.silu(g) * up).astype(BF16)
            c = pl.ds(pl.multiple_of(i * 128, 128), 128)
            u[pl.ds(pl.multiple_of(top * blk, blk), half), c] = val[:half]
            u[pl.ds(pl.multiple_of(bottom * blk + half, half), half), c] = val[half:]

    def rows_of_u(top, bottom):
        return lambda: jnp.concatenate([u[pl.ds(pl.multiple_of(top * blk, blk), half), :],
                                        u[pl.ds(pl.multiple_of(bottom * blk + half, half), half), :]], axis=0)

    down_pieces = (lambda top, bottom, z: project(rows_of_u(top, bottom), wd, z, 0, tiles // 2),
                   lambda top, bottom, z: project(rows_of_u(top, bottom), wd, z, tiles // 2, tiles))
    cut = ff // 128 // 2

    first = n - 1
    halves = ((0, cut), (cut, ff // 128))

    def gate_up_of(j, s):
        gate_up(*halves[j], slots.at[lax.rem(first + s, SLOTS)], lax.rem(me + n - s - 1, n), lax.rem(me + s + 1, n))

    all_gather(1, lambda: gate_up(0, ff // 128, stage, me, me),
               lambda j, s: pl.when(s >= 1)(lambda: gate_up_of(j, s - 1)), last - 1)

    for d in range(2):
        take_credit(d, first + last)
    reduce_start(2, down_pieces)
    m13, m14 = first + last - 1, first + last
    for j, d in pairs:
        message(d, j, m13).wait_recv()
        pl.when(stays[d])(lambda d=d, j=j: message(d, j, m14, slots.at[m13 % SLOTS, rows(d, j)]).start())
        if d == 1:
            gate_up_of(j, last - 2)

    def begin(s):
        @pl.when(s == 1)
        def _():
            for j, d in pairs:
                last_arrival(d, j, 1)

    def extra(s, j):
        pl.when(s == 0)(lambda: gate_up_of(j, last - 1))
        pl.when(s == 1)(lambda: gate_up_of(j, last))

    def end(s):
        @pl.when(s == 0)
        def _():
            for j, d in pairs:
                message(d, j, m13).wait_send()
            give_credit(m13 - 1)
            for j, d in pairs:
                pl.when(stays[d])(lambda d=d, j=j: message(d, j, m14).wait_send())
            give_credit(m13)

        @pl.when(s == 1)
        def _():
            give_credit(m14)

    def finish_y(r, total):
        stage[r, :] = (hown[r, :].astype(F32) + total).astype(BF16)

    reduce_scatter(2, down_pieces, finish_y, begin, extra, end)

    def own():
        y[pl.ds(pl.multiple_of(me * blk, blk), blk), :] = stage[...]

    def store(j, slot, top, bottom):
        for d, block in enumerate((top, bottom)):
            at = pl.multiple_of(block * blk + d * half + j * sub, sub)
            y[pl.ds(at, sub), :] = slots[slot, span(d, j), :]

    base = 3 * (n - 1)
    all_gather(3, own, lambda j, s: store(j, lax.rem(base + s, SLOTS), lax.rem(me + n - s - 1, n),
                                          lax.rem(me + s + 1, n)), last)
    m = base + last
    for j, d in pairs:
        last_arrival(d, j, 3)
        if d == 1:
            store(j, m % SLOTS, right, left)
    for j, d in pairs:
        pl.when(stays[d])(lambda d=d, j=j: message(d, j, m).wait_send())
    give_credit(m - 1)
    give_credit(m)


def _ring(n, q, k, v, x, g2, wo, wg, wu, wd):
    t, d = x.shape
    ff = wd.shape[0]
    blk = t // n
    hbm = pl.BlockSpec(memory_space=pl.ANY)
    dma = pltpu.SemaphoreType.DMA
    return pl.pallas_call(
        functools.partial(_ring_kernel, n),
        out_shape=pltpu.VMEM((t, d), BF16),
        in_specs=[hbm] * 4 + [pl.BlockSpec(memory_space=pltpu.VMEM)] + [hbm] * 4,
        out_specs=pl.BlockSpec(memory_space=pltpu.VMEM),
        scratch_shapes=[
            pltpu.VMEM((SLOTS, blk, d), BF16),
            pltpu.VMEM((4, blk // 2, d), BF16),
            pltpu.VMEM((blk, d), BF16),
            pltpu.VMEM((2, blk, d), F32),
            pltpu.VMEM((blk, d), BF16),
            pltpu.VMEM((t, ff), BF16),
            pltpu.VMEM(q.shape, BF16),
            pltpu.VMEM(k.shape, BF16),
            pltpu.VMEM(v.shape, BF16),
            pltpu.VMEM((blk * (q.shape[1] // HEAD), t), F32),
            pltpu.VMEM((blk * (q.shape[1] // HEAD), 128), F32),
            pltpu.VMEM((blk, q.shape[1]), BF16),
            pltpu.VMEM(wo.shape, BF16),
            pltpu.VMEM((d, 2 * ff), BF16),
            pltpu.VMEM(wd.shape, BF16),
            dma((2, SUBS, SLOTS)),
            dma((2, SUBS, SLOTS)),
            dma((4, SUBS)),
            dma((4, SUBS)),
            dma((6 + 2 * (ff // 128),)),
            pltpu.SemaphoreType.REGULAR((2,)),
        ],
        compiler_params=pltpu.CompilerParams(
            collective_id=0, has_side_effects=True, vmem_limit_bytes=VMEM_RING),
        name="ring_layer",
    )(q, k, v, x, g2, wo, wg, wu, wd)


def _store_kernel(y_vmem, y_hbm, sem):
    parts = 8
    r = y_vmem.shape[0] // parts
    copies = [pltpu.make_async_copy(y_vmem.at[pl.ds(i * r, r)], y_hbm.at[pl.ds(i * r, r)], sem.at[i])
              for i in range(parts)]
    for cp in copies:
        cp.start()
    for cp in copies:
        cp.wait()


def _store(y):
    return pl.pallas_call(
        _store_kernel,
        out_shape=jax.ShapeDtypeStruct(y.shape, y.dtype),
        in_specs=[pl.BlockSpec(memory_space=pltpu.VMEM)],
        out_specs=pl.BlockSpec(memory_space=pl.ANY),
        scratch_shapes=[pltpu.SemaphoreType.DMA((8,))],
        compiler_params=pltpu.CompilerParams(vmem_limit_bytes=4 << 20),
        name="store",
    )(y)


def solution(mesh):
    tp = mesh.shape["tp"]

    def local(x, pos, g1, g2, wq, wk, wv, wo, wg, wu, wd):
        t, d = x.shape
        g = wk.shape[1] // HEAD
        r = lax.axis_index("tp")
        head = (r * g // tp).astype(jnp.int32).reshape(1)
        half = HEAD // 2
        inv = ROPE_BASE ** (-2.0 * jnp.arange(half, dtype=F32) / HEAD)
        ang = pos.astype(F32)[:, None] * inv
        c, s = jnp.cos(ang), jnp.sin(ang)
        cos = jnp.concatenate([c, c], axis=-1)
        sin = jnp.concatenate([-s, s], axis=-1)
        q, k, v = _qkv(head, x, g1.reshape(1, d), cos, sin, wq, wk, wv)
        y = _store(_ring(tp, q, k, v, x, g2.reshape(1, d), wo, wg, wu, wd))
        return y, k.reshape(t, 1, HEAD), v.reshape(t, 1, HEAD)

    return jax.shard_map(
        local,
        mesh=mesh,
        in_specs=(P("dp", None), P("dp"), P(), P(), P(None, "tp"), P(), P(), P("tp", None),
                  P(None, "tp"), P(None, "tp"), P("tp", None)),
        out_specs=(P("dp", None), P("dp", "tp", None), P("dp", "tp", None)),
        check_vma=False,
    )
```

```python
import functools

import jax
import jax.numpy as jnp
from jax import lax
from jax.experimental import pallas as pl
from jax.experimental.pallas import tpu as pltpu
from jax.sharding import PartitionSpec as P

HEAD = 128
EPS = 1e-5
ROPE_BASE = 500000.0
SLOTS = 6
SUBS = 2
VMEM_RING = 50 * 10**6
MESH = pl.DeviceIdType.MESH
F32, BF16 = jnp.float32, jnp.bfloat16


def _qkv_kernel(hd_ref, x_ref, g1_ref, cos_ref, sin_ref, wq_ref, wk_ref, wv_ref,
                q_ref, k_ref, v_ref, wkv, a0, a1):
    i = pl.program_id(0)
    steps = pl.num_programs(0)
    hb, d = a0.shape
    hl = wq_ref.shape[1] // HEAD
    chunks = 4
    rows = hb // chunks
    kd = d // chunks

    def norm(x0, a, z):
        r = slice(x0 + z * rows, x0 + (z + 1) * rows)
        o = slice(z * rows, (z + 1) * rows)
        ss = None
        for t in range(d // 128):
            x32 = x_ref[r, t * 128:(t + 1) * 128].astype(F32)
            ss = x32 * x32 if ss is None else ss + x32 * x32
        inv = lax.rsqrt(jnp.sum(ss, axis=-1, keepdims=True) * (1.0 / d) + EPS)
        for t in range(d // 128):
            c = slice(t * 128, (t + 1) * 128)
            a[o, c] = (x_ref[r, c].astype(F32) * inv * g1_ref[t:t + 1, :].astype(F32)).astype(BF16)

    def work(a, at, x0=None, into=None):
        kv = q = None
        for z in range(chunks):
            kk = slice(z * kd, (z + 1) * kd)
            t = jnp.dot(a[:, kk], wkv[kk, :], preferred_element_type=F32)
            kv = t if kv is None else kv + t
            t = jnp.dot(a[:, kk], wq_ref[kk, :], preferred_element_type=F32)
            q = t if q is None else q + t
            if into is not None:
                norm(x0, into, z)
        here = pl.ds(pl.multiple_of(at, hb), hb)
        c, s = cos_ref[here, :], sin_ref[here, :]

        def rope(t):
            return (t * c + pltpu.roll(t, HEAD // 2, 1) * s).astype(BF16)

        k_ref[here, :] = rope(kv[:, :HEAD])
        v_ref[here, :] = kv[:, HEAD:].astype(BF16)
        for h in range(hl):
            q_ref[here, h * HEAD:(h + 1) * HEAD] = rope(q[:, h * HEAD:(h + 1) * HEAD])

    @pl.when(i == 0)
    def _():
        wkv[:, :HEAD] = wk_ref[...]
        wkv[:, HEAD:] = wv_ref[...]
        for z in range(chunks):
            norm(0, a0, z)

    @pl.when(jnp.logical_and(i > 0, i < steps - 1))
    def _():
        work(a1, (2 * i - 1) * hb, 0, a0)

    @pl.when(i < steps - 1)
    def _():
        work(a0, 2 * i * hb, hb, a1)

    @pl.when(i == steps - 1)
    def _():
        work(a1, (2 * i - 1) * hb)


def _qkv(head, x, g1, cos, sin, wq, wk, wv):
    t, d = x.shape
    hb = min(t // 4, 256)
    nb = t // (2 * hb)
    hw = wq.shape[1]
    spec = pltpu.PrefetchScalarGridSpec(
        num_scalar_prefetch=1,
        grid=(nb + 1,),
        in_specs=[
            pl.BlockSpec((2 * hb, d), lambda i, hd: (jnp.minimum(i, nb - 1), 0)),
            pl.BlockSpec((d // 128, 128), lambda i, hd: (0, 0)),
            pl.BlockSpec((t, HEAD), lambda i, hd: (0, 0)),
            pl.BlockSpec((t, HEAD), lambda i, hd: (0, 0)),
            pl.BlockSpec((d, hw), lambda i, hd: (0, 0)),
            pl.BlockSpec((d, HEAD), lambda i, hd: (0, hd[0])),
            pl.BlockSpec((d, HEAD), lambda i, hd: (0, hd[0])),
        ],
        out_specs=[
            pl.BlockSpec((t, hw), lambda i, hd: (0, 0)),
            pl.BlockSpec((t, HEAD), lambda i, hd: (0, 0)),
            pl.BlockSpec((t, HEAD), lambda i, hd: (0, 0)),
        ],
        scratch_shapes=[
            pltpu.VMEM((d, 2 * HEAD), BF16),
            pltpu.VMEM((hb, d), BF16),
            pltpu.VMEM((hb, d), BF16),
        ],
    )
    return pl.pallas_call(
        _qkv_kernel,
        out_shape=(jax.ShapeDtypeStruct((t, hw), BF16), jax.ShapeDtypeStruct((t, HEAD), BF16),
                   jax.ShapeDtypeStruct((t, HEAD), BF16)),
        grid_spec=spec,
        compiler_params=pltpu.CompilerParams(
            dimension_semantics=("arbitrary",), vmem_limit_bytes=48 << 20),
        name="qkv",
    )(head, x, g1, cos, sin, wq, wk, wv)


def _ring_kernel(n, q_hbm, k_hbm, v_hbm, x_hbm, g2_ref, wo_hbm, wg_hbm, wu_hbm, wd_hbm, y,
                 slots, early, stage, part, hown, u, q, k, v, sc, top_score, orow, wo, wgu, wd,
                 send_sem, recv_sem, early_send, early_recv, in_sem, free_sem):
    me = lax.axis_index("tp")
    right, left = lax.rem(me + 1, n), lax.rem(me + n - 1, n)
    peer = (right, left)
    odd = lax.rem(me, 2)
    leaves = (odd == 1, odd == 0)
    stays = (odd == 0, odd == 1)
    d_model = wo.shape[1]
    ff = wd.shape[0]
    t_all = q.shape[0]
    heads = q.shape[1] // HEAD
    blk = stage.shape[0]
    half = blk // 2
    sub = half // SUBS
    last = n - 2
    total_msgs = 4 * (n - 1)
    pairs = [(j, d) for j in range(SUBS) for d in range(2)]

    loads = [pltpu.make_async_copy(src, dst, in_sem.at[i]) for i, (src, dst) in enumerate([
        (q_hbm, q), (k_hbm, k), (v_hbm, v), (wo_hbm, wo),
        (x_hbm.at[pl.ds(pl.multiple_of(me * blk, blk), blk)], hown), (wd_hbm, wd)])]
    for i in range(ff // 128):
        c = pl.ds(i * 128, 128)
        loads.append(pltpu.make_async_copy(wg_hbm.at[:, c], wgu.at[:, pl.ds(i * 256, 128)], in_sem.at[6 + 2 * i]))
        loads.append(pltpu.make_async_copy(wu_hbm.at[:, c], wgu.at[:, pl.ds(i * 256 + 128, 128)], in_sem.at[7 + 2 * i]))
    for cp in loads[:5]:
        cp.start()

    barrier = pltpu.get_barrier_semaphore()
    for p in peer:
        pl.semaphore_signal(barrier, inc=1, device_id={"tp": p}, device_id_type=MESH)

    def rows(d, j):
        return pl.ds(d * half + j * sub, sub)

    def span(d, j):
        return slice(d * half + j * sub, d * half + (j + 1) * sub)

    def message(d, j, m, src=None):
        slot = lax.rem(m, SLOTS)
        dst = slots.at[slot, rows(d, j)]
        return pltpu.make_async_remote_copy(
            src_ref=dst if src is None else src, dst_ref=dst,
            send_sem=send_sem.at[d, j, slot], recv_sem=recv_sem.at[d, j, slot],
            device_id={"tp": peer[d]}, device_id_type=MESH)

    def direct(d, j, phase):
        return pltpu.make_async_remote_copy(
            src_ref=stage.at[rows(d, j)], dst_ref=early.at[phase, pl.ds(j * sub, sub)],
            send_sem=early_send.at[phase, j], recv_sem=early_recv.at[phase, j],
            device_id={"tp": peer[1 - d]}, device_id_type=MESH)

    def when(cond, fn):
        if isinstance(cond, bool):
            if cond:
                fn()
        else:
            pl.when(cond)(fn)

    def take_credit(d, m):
        when(m >= SLOTS, lambda: pl.semaphore_wait(free_sem.at[d], 1))

    def give_credit(m):
        for d in range(2):
            when(m <= total_msgs - 1 - SLOTS, functools.partial(
                pl.semaphore_signal, free_sem.at[d], inc=1, device_id={"tp": peer[1 - d]}, device_id_type=MESH))

    tile = min(512, d_model // 2)

    tiles = d_model // tile

    def project(lhs, w, z, first, stop):
        @pl.loop(first, stop)
        def _(i):
            c = pl.ds(pl.multiple_of(i * tile, tile), tile)
            part[z, :, c] = jnp.dot(lhs(), w[:, c], preferred_element_type=F32)

    def reduce_start(phase, pieces):
        base = phase * (n - 1)
        for piece in pieces:
            piece(left, right, 1)
        stage[...] = part[1].astype(BF16)
        for j, d in pairs:
            if j == 0:
                take_credit(d, base)
            pl.when(leaves[d])(lambda d=d, j=j: direct(d, j, phase).start())
            pl.when(stays[d])(lambda d=d, j=j: message(d, j, base, stage.at[rows(d, j)]).start())
        for piece in pieces:
            piece(lax.rem(me + n - 2, n), lax.rem(me + 2, n), 0)

    def forward(d, j, m, ref):
        if j == 0:
            take_credit(d, m)
        message(d, j, m, ref).start()

    def add_and_forward(d, j, m, z):
        message(d, j, m).wait_recv()
        ref = slots.at[lax.rem(m, SLOTS), rows(d, j)]
        ref[...] = (ref[...].astype(F32) + part[z, span(d, j), :]).astype(BF16)
        forward(d, j, m + 1, ref)

    def reduce_scatter(phase, pieces, finish, begin=None, extra=None, end=None):
        base = phase * (n - 1)

        @pl.loop(0, last)
        def _(s):
            m = base + s
            slot = lax.rem(m, SLOTS)
            z = lax.rem(s, 2)
            top, bottom = lax.rem(me + 2 * n - s - 3, n), lax.rem(me + s + 3, n)
            if begin is not None:
                begin(s)
            for j, d in pairs:
                ref = slots.at[slot, rows(d, j)]
                opens = jnp.logical_and(s == 0, stays[d])

                @pl.when(opens)
                def _():
                    ref[...] = part[z, span(d, j), :].astype(BF16)

                @pl.when(s >= 1 if phase == 0 else jnp.logical_not(opens))
                def _():
                    add_and_forward(d, j, m, z)

                @pl.when(opens)
                def _():
                    forward(d, j, m + 1, ref)
                if d == 1:
                    pieces[j](top, bottom, 1 - z)
                    if extra is not None:
                        extra(s, j)
            for j, d in pairs:
                handed = jnp.logical_and(s == 0, leaves[d])
                pl.when(handed)(lambda d=d, j=j: direct(d, j, phase).wait_send())
                pl.when(jnp.logical_not(handed))(lambda d=d, j=j: message(d, j, m).wait_send())
            if end is not None:
                end(s)
            pl.when(s >= 1)(lambda: give_credit(m - 1))

        m = base + last
        z = last % 2
        for j, d in pairs:
            @pl.when(stays[d])
            def _():
                direct(d, j, phase).wait_recv()
                part[z, span(d, j), :] = part[z, span(d, j), :] + early[phase, j * sub:(j + 1) * sub, :].astype(F32)
        for j, d in pairs:
            message(d, j, m).wait_recv()
            r = span(d, j)
            finish(r, slots[m % SLOTS, r, :].astype(F32) + part[z, r, :])
            if j == 0:
                take_credit(d, m + 1)
            message(d, j, m + 1, stage.at[rows(d, j)]).start()
            pl.when(leaves[d])(lambda d=d, j=j: direct(d, j, phase + 1).start())
        for j, d in pairs:
            message(d, j, m).wait_send()
        give_credit(m - 1)
        give_credit(m)

    def last_arrival(d, j, phase):
        m = phase * (n - 1) + last

        @pl.when(leaves[d])
        def _():
            message(d, j, m).wait_recv()

        @pl.when(stays[d])
        def _():
            direct(d, j, phase).wait_recv()
            slots[m % SLOTS, span(d, j), :] = early[phase, j * sub:(j + 1) * sub, :]

    def all_gather(phase, own, arrived, stop):
        base = phase * (n - 1)
        own()

        @pl.loop(0, stop)
        def _(s):
            m = base + s
            slot = lax.rem(m, SLOTS)
            for j, d in pairs:
                message(d, j, m).wait_recv()
                if j == 0:
                    take_credit(d, m + 1)
                onward = functools.partial(lambda d, j: message(d, j, m + 1, slots.at[slot, rows(d, j)]).start(), d, j)
                if stop < last:
                    onward()
                else:
                    pl.when(jnp.logical_or(s < last - 1, stays[d]))(onward)
                if d == 1:
                    arrived(j, s)
            for j, d in pairs:
                message(d, j, m).wait_send()
                pl.when(jnp.logical_and(s == 0, leaves[d]))(lambda d=d, j=j: direct(d, j, phase).wait_send())
            pl.when(s >= 1)(lambda: give_credit(m - 1))

    kt = min(256, t_all)
    scale = HEAD ** -0.5
    lanes = kt // 128

    def attend_scores(top, bottom, z):
        r0 = pl.multiple_of(top * blk, half)
        r1 = pl.multiple_of(bottom * blk + half, half)
        qa, qb = q[pl.ds(r0, half), :], q[pl.ds(r1, half), :]
        qq = jnp.concatenate([t[:, h * HEAD:(h + 1) * HEAD] for t in (qa, qb) for h in range(heads)], axis=0)
        i = lax.broadcasted_iota(jnp.int32, (2 * heads * half, kt), 0)
        row = jnp.where(i < heads * half, r0, r1) + (i & (half - 1))
        ahead = row - lax.broadcasted_iota(jnp.int32, row.shape, 1)
        mx = None
        for b in range(t_all // kt):
            c = slice(b * kt, (b + 1) * kt)
            t = lax.dot_general(qq, k[c, :], (((1,), (1,)), ((), ())), preferred_element_type=F32) * scale
            t = jnp.where(ahead >= b * kt, t, -jnp.inf)
            sc[:, c] = t
            for y in range(lanes):
                g = t[:, y * 128:(y + 1) * 128]
                mx = g if mx is None else jnp.maximum(mx, g)
        top_score[...] = jnp.broadcast_to(jnp.max(mx, axis=-1, keepdims=True), mx.shape)

    def attend_values(top, bottom, z):
        mx = top_score[...]
        tot = None
        for b in range(t_all // 128):
            c = slice(b * 128, (b + 1) * 128)
            e = jnp.exp(sc[:, c] - mx)
            sc[:, c] = e
            tot = e if tot is None else tot + e
        rinv = 1.0 / jnp.sum(tot, axis=-1, keepdims=True)
        acc = None
        for b in range(t_all // kt):
            c = slice(b * kt, (b + 1) * kt)
            pr = (sc[:, c] * rinv).astype(BF16)
            g = jnp.dot(pr, v[c, :], preferred_element_type=F32)
            acc = g if acc is None else acc + g
        for y in range(2):
            for h in range(heads):
                w = y * heads + h
                orow[y * half:(y + 1) * half, h * HEAD:(h + 1) * HEAD] = acc[w * half:(w + 1) * half].astype(BF16)
        project(lambda: orow[...], wo, z, 0, tiles)

    output_pieces = (attend_scores, attend_values)


    def finish_h(r, total):
        h = (hown[r, :].astype(F32) + total).astype(BF16)
        hown[r, :] = h
        h32 = h.astype(F32)
        inv = lax.rsqrt(jnp.mean(h32 * h32, axis=-1, keepdims=True) + EPS)
        gain = jnp.concatenate([g2_ref[t:t + 1, :].astype(F32) for t in range(d_model // 128)], axis=1)
        stage[r, :] = (h32 * inv * gain).astype(BF16)

    def by_parity(a, b):
        return lax.rem(jnp.where(odd == 1, a, b), n)

    def cast_to_stage(d, z):
        for j in range(SUBS):
            stage[rows(d, j), :] = part[z, span(d, j), :].astype(BF16)

    top, bottom = by_parity(me + n - 2, me + n - 1), by_parity(me + 1, me + 2)
    for cp in loads[:2]:
        cp.wait()
    attend_scores(top, bottom, 0)
    for cp in loads[2:4]:
        cp.wait()
    for cp in loads[5:]:
        cp.start()
    attend_values(top, bottom, 0)
    pl.semaphore_wait(barrier, 2)
    for d in range(2):
        @pl.when(stays[d])
        def _():
            cast_to_stage(d, 0)
            for j in range(SUBS):
                message(d, j, 0, stage.at[rows(d, j)]).start()
    for d in range(2):
        @pl.when(leaves[d])
        def _():
            for j in range(SUBS):
                add_and_forward(d, j, 0, 0)
    top, bottom = by_parity(me + n - 1, me + n - 2), by_parity(me + 2, me + 1)
    attend_scores(top, bottom, 1)
    attend_values(top, bottom, 1)
    for d in range(2):
        @pl.when(leaves[d])
        def _():
            cast_to_stage(d, 1)
            for j in range(SUBS):
                direct(d, j, 0).start()

        @pl.when(stays[d])
        def _():
            for j in range(SUBS):
                part[0, span(d, j), :] = part[1, span(d, j), :]
    loads[4].wait()
    reduce_scatter(0, output_pieces, finish_h)

    for cp in loads[5:]:
        cp.wait()

    def gate_up(first, stop, b_ref, top, bottom):
        @pl.loop(first, stop)
        def _(i):
            gu = jnp.dot(b_ref[...], wgu[:, pl.ds(pl.multiple_of(i * 256, 256), 256)], preferred_element_type=F32)
            g, up = gu[:, :128], gu[:, 128:]
            val = (jax.nn.silu(g) * up).astype(BF16)
            c = pl.ds(pl.multiple_of(i * 128, 128), 128)
            u[pl.ds(pl.multiple_of(top * blk, blk), half), c] = val[:half]
            u[pl.ds(pl.multiple_of(bottom * blk + half, half), half), c] = val[half:]

    def rows_of_u(top, bottom):
        return lambda: jnp.concatenate([u[pl.ds(pl.multiple_of(top * blk, blk), half), :],
                                        u[pl.ds(pl.multiple_of(bottom * blk + half, half), half), :]], axis=0)

    down_pieces = (lambda top, bottom, z: project(rows_of_u(top, bottom), wd, z, 0, tiles // 2),
                   lambda top, bottom, z: project(rows_of_u(top, bottom), wd, z, tiles // 2, tiles))
    cut = ff // 128 // 2

    first = n - 1
    halves = ((0, cut), (cut, ff // 128))

    def gate_up_of(j, s):
        gate_up(*halves[j], slots.at[lax.rem(first + s, SLOTS)], lax.rem(me + n - s - 1, n), lax.rem(me + s + 1, n))

    all_gather(1, lambda: gate_up(0, ff // 128, stage, me, me),
               lambda j, s: pl.when(s >= 1)(lambda: gate_up_of(j, s - 1)), last - 1)

    for d in range(2):
        take_credit(d, first + last)
    reduce_start(2, down_pieces)
    m13, m14 = first + last - 1, first + last
    for j, d in pairs:
        message(d, j, m13).wait_recv()
        pl.when(stays[d])(lambda d=d, j=j: message(d, j, m14, slots.at[m13 % SLOTS, rows(d, j)]).start())
        if d == 1:
            gate_up_of(j, last - 2)

    def begin(s):
        @pl.when(s == 1)
        def _():
            for j, d in pairs:
                last_arrival(d, j, 1)

    def extra(s, j):
        pl.when(s == 0)(lambda: gate_up_of(j, last - 1))
        pl.when(s == 1)(lambda: gate_up_of(j, last))

    def end(s):
        @pl.when(s == 0)
        def _():
            for j, d in pairs:
                message(d, j, m13).wait_send()
            give_credit(m13 - 1)
            for j, d in pairs:
                pl.when(stays[d])(lambda d=d, j=j: message(d, j, m14).wait_send())
            give_credit(m13)

        @pl.when(s == 1)
        def _():
            give_credit(m14)

    def finish_y(r, total):
        stage[r, :] = (hown[r, :].astype(F32) + total).astype(BF16)

    reduce_scatter(2, down_pieces, finish_y, begin, extra, end)

    def own():
        y[pl.ds(pl.multiple_of(me * blk, blk), blk), :] = stage[...]

    def store(j, slot, top, bottom):
        for d, block in enumerate((top, bottom)):
            at = pl.multiple_of(block * blk + d * half + j * sub, sub)
            y[pl.ds(at, sub), :] = slots[slot, span(d, j), :]

    base = 3 * (n - 1)
    all_gather(3, own, lambda j, s: store(j, lax.rem(base + s, SLOTS), lax.rem(me + n - s - 1, n),
                                          lax.rem(me + s + 1, n)), last)
    m = base + last
    for j, d in pairs:
        last_arrival(d, j, 3)
        if d == 1:
            store(j, m % SLOTS, right, left)
    for j, d in pairs:
        pl.when(stays[d])(lambda d=d, j=j: message(d, j, m).wait_send())
    give_credit(m - 1)
    give_credit(m)


def _ring(n, q, k, v, x, g2, wo, wg, wu, wd):
    t, d = x.shape
    ff = wd.shape[0]
    blk = t // n
    hbm = pl.BlockSpec(memory_space=pl.ANY)
    dma = pltpu.SemaphoreType.DMA
    return pl.pallas_call(
        functools.partial(_ring_kernel, n),
        out_shape=pltpu.VMEM((t, d), BF16),
        in_specs=[hbm] * 4 + [pl.BlockSpec(memory_space=pltpu.VMEM)] + [hbm] * 4,
        out_specs=pl.BlockSpec(memory_space=pltpu.VMEM),
        scratch_shapes=[
            pltpu.VMEM((SLOTS, blk, d), BF16),
            pltpu.VMEM((4, blk // 2, d), BF16),
            pltpu.VMEM((blk, d), BF16),
            pltpu.VMEM((2, blk, d), F32),
            pltpu.VMEM((blk, d), BF16),
            pltpu.VMEM((t, ff), BF16),
            pltpu.VMEM(q.shape, BF16),
            pltpu.VMEM(k.shape, BF16),
            pltpu.VMEM(v.shape, BF16),
            pltpu.VMEM((blk * (q.shape[1] // HEAD), t), F32),
            pltpu.VMEM((blk * (q.shape[1] // HEAD), 128), F32),
            pltpu.VMEM((blk, q.shape[1]), BF16),
            pltpu.VMEM(wo.shape, BF16),
            pltpu.VMEM((d, 2 * ff), BF16),
            pltpu.VMEM(wd.shape, BF16),
            dma((2, SUBS, SLOTS)),
            dma((2, SUBS, SLOTS)),
            dma((4, SUBS)),
            dma((4, SUBS)),
            dma((6 + 2 * (ff // 128),)),
            pltpu.SemaphoreType.REGULAR((2,)),
        ],
        compiler_params=pltpu.CompilerParams(
            collective_id=0, has_side_effects=True, vmem_limit_bytes=VMEM_RING),
        name="ring_layer",
    )(q, k, v, x, g2, wo, wg, wu, wd)


def _store_kernel(y_vmem, y_hbm, sem):
    parts = 8
    r = y_vmem.shape[0] // parts
    copies = [pltpu.make_async_copy(y_vmem.at[pl.ds(i * r, r)], y_hbm.at[pl.ds(i * r, r)], sem.at[i])
              for i in range(parts)]
    for cp in copies:
        cp.start()
    for cp in copies:
        cp.wait()


def _store(y):
    return pl.pallas_call(
        _store_kernel,
        out_shape=jax.ShapeDtypeStruct(y.shape, y.dtype),
        in_specs=[pl.BlockSpec(memory_space=pltpu.VMEM)],
        out_specs=pl.BlockSpec(memory_space=pl.ANY),
        scratch_shapes=[pltpu.SemaphoreType.DMA((8,))],
        compiler_params=pltpu.CompilerParams(vmem_limit_bytes=4 << 20),
        name="store",
    )(y)


def solution(mesh):
    tp = mesh.shape["tp"]

    def local(x, pos, g1, g2, wq, wk, wv, wo, wg, wu, wd):
        t, d = x.shape
        g = wk.shape[1] // HEAD
        r = lax.axis_index("tp")
        head = (r * g // tp).astype(jnp.int32).reshape(1)
        half = HEAD // 2
        inv = ROPE_BASE ** (-2.0 * jnp.arange(half, dtype=F32) / HEAD)
        ang = pos[:, None].astype(F32) * inv
        c, s = jnp.cos(ang), jnp.sin(ang)
        cos = jnp.concatenate([c, c], axis=-1)
        sin = jnp.concatenate([-s, s], axis=-1)
        q, k, v = _qkv(head, x, g1.reshape(d // 128, 128), cos, sin, wq, wk, wv)
        y = _store(_ring(tp, q, k, v, x, g2.reshape(d // 128, 128), wo, wg, wu, wd))
        return y, k.reshape(t, 1, HEAD), v.reshape(t, 1, HEAD)

    return jax.shard_map(
        local,
        mesh=mesh,
        in_specs=(P("dp", None), P("dp"), P(), P(), P(None, "tp"), P(), P(), P("tp", None),
                  P(None, "tp"), P(None, "tp"), P("tp", None)),
        out_specs=(P("dp", None), P("dp", "tp", None), P("dp", "tp", None)),
        check_vma=False,
    )
```
